32 devices in a mesh: dp: 8 (over z, x), tensor: 4 (over y, core).
Axes of the slice: x: 2, y: 2, z: 4, core: 2. Of those that a mesh axis runs over, the one named last changes fastest.
Arguments:
- block_input: float32 [8, 1280, 768], P('dp', 'tensor'), may hold values from -6 to 6
- passes: int32 [8], P('dp'), may hold values from 2 to 5, as said below
- pass_map: int32 [8, 1280], P('dp', 'tensor'), may hold values from 0 to 4, as said below
- pass_table: float32 [5, 768], replicated, may hold values from -5 to 5
- gain_one: float32 [768], replicated, may hold values from 0.1 to 1.9
- bias_one: float32 [768], replicated, may hold values from -3 to 3
- w_qkv: float32 [768, 3, 768], P(None, None, 'tensor'), may hold values from -0.21875 to 0.21875
- w_out: float32 [768, 768], P('tensor'), may hold values from -4 to 4
- gain_two: float32 [768], replicated, may hold values from 0.1 to 1.9
- bias_two: float32 [768], replicated, may hold values from -3 to 3
- w_up: float32 [768, 3072], P(None, 'tensor'), may hold values from -0.21875 to 0.21875
- w_down: float32 [3072, 768], P('tensor'), may hold values from -0.109375 to 0.109375
- grad_output: float32 [8, 1280, 768], P('dp', 'tensor'), may hold values from -6 to 6
Outputs:
- block_output: float32 [8, 1280, 768], P('dp', 'tensor')
- grad_input: float32 [8, 1280, 768], P('dp', 'tensor')
- grad_table: float32 [5, 768], P(None, 'dp')
- grad_gain_one: float32 [768], P('dp')
- grad_bias_one: float32 [768], P('dp')
- grad_qkv: float32 [768, 3, 768], P('dp', None, 'tensor')
- grad_out: float32 [768, 768], P('tensor', 'dp')
- grad_gain_two: float32 [768], P('dp')
- grad_bias_two: float32 [768], P('dp')
- grad_up: float32 [768, 3072], P('dp', 'tensor')
- grad_down: float32 [3072, 768], P('tensor', 'dp')
The draws below stay inside these ranges and needn't reach their ends.
Inputs may be any that keep to these rules, and one draw needn't show every extreme that they name: Every draw has an item with 5 passes and an item with 2 passes. `pass_map`: slot s of an item with r passes holds s mod r.
All inputs are finite; a program needn't handle non-finite values.
Results may differ from the reference program's by a relative error of at most 0.0003.
Values sent between devices are 32-bit elements; how exact they have to be, the bound alone decides.
A program may use at most 128 MiB of HBM per device.

```python
import math
import jax
import jax.numpy as jnp
from jax import lax

D = 768
HEADS = 12
HD = 64
FF = 3072
BASE = 256
PASSES_MAX = 5
SLOTS = 1280
ITEMS = 8


def pass_counts(key):
    counts = jax.random.randint(jax.random.fold_in(key, 11), (ITEMS,), 2, PASSES_MAX + 1)
    order = jax.random.permutation(jax.random.fold_in(key, 12), ITEMS)
    counts = counts.at[order[0]].set(PASSES_MAX).at[order[1]].set(2)
    return counts.astype(jnp.int32)


def draw_passes(key, part):
    return pass_counts(key)


def draw_pass_map(key, part):
    counts = pass_counts(key)
    return (jnp.arange(SLOTS)[None, :] % counts[:, None]).astype(jnp.int32)


def strengthened(values, own_key, source, target, blocks, factor):
    def block_of(position):
        return (jnp.arange(values.shape[position]) // (values.shape[position] // blocks)).reshape((-1,) + (1,) * (values.ndim - 1 - position))

    one_side = jax.random.permutation(own_key, blocks)[block_of(target)]
    second = (block_of(target) + blocks // 2) % blocks
    return jnp.where((block_of(source) == one_side) | (block_of(source) == second), factor * values, values)


def levels(key, extent, pieces, least, largest):
    factor_of = 1.0
    for dim, blocks in pieces:
        steps = jax.random.uniform(jax.random.fold_in(jax.random.fold_in(key, 6), dim), (blocks,), jnp.float32, least / len(pieces), largest / len(pieces))
        factor_of = factor_of * jnp.repeat(jnp.exp(steps), extent[dim] // blocks).reshape((-1,) + (1,) * (len(extent) - 1 - dim))
    return factor_of


def noise(rng, shape, width, reach, shards=(), dtype=jnp.bfloat16):
    level = levels(rng, shape, shards, -0.22, 0.18) if shards else 1.0
    array = jax.random.normal(rng, shape, jnp.float32) * width * level
    return jnp.minimum(jnp.maximum(array, -reach), reach).astype(dtype)


def noise_with(own_key, dims, scale, bound, shards, heavy, held_as=jnp.bfloat16):
    array = scale * jax.random.normal(own_key, dims, jnp.float32)
    if shards:
        array = array * levels(own_key, dims, shards, -0.22, 0.18)
    return jnp.clip(strengthened(array, jax.random.fold_in(own_key, 3), *heavy), -bound, bound).astype(held_as)


def setup_inputs(seed: int = 0) -> dict:
    arg_keys = jax.random.split(jax.random.key(seed), 14)
    return {
        "block_input": noise(arg_keys[0], (ITEMS, SLOTS, D), 1.0, 6.0, ((0, 8), (1, 4)), jnp.float32),
        "passes": draw_passes(jax.random.fold_in(arg_keys[13], 71), 0),
        "pass_map": draw_pass_map(jax.random.fold_in(arg_keys[13], 71), 0),
        "pass_table": noise(arg_keys[3], (PASSES_MAX, D), 1.0, 5.0, (), jnp.float32),
        "gain_one": jnp.clip(1.0 + 0.18 * jax.random.normal(arg_keys[4], (D,), jnp.float32), 0.1, 1.9),
        "bias_one": noise(arg_keys[5], (D,), 0.5, 3.0, (), jnp.float32),
        "w_qkv": noise(arg_keys[6], (D, 3, D), D ** -0.5, 0.21875, ((2, 4),), jnp.float32),
        "w_out": noise(arg_keys[7], (D, D), 2 ** -0.5, 4.0, ((0, 4),), jnp.float32),
        "gain_two": jnp.clip(1.0 + 0.18 * jax.random.normal(arg_keys[8], (D,), jnp.float32), 0.1, 1.9),
        "bias_two": noise(arg_keys[9], (D,), 0.5, 3.0, (), jnp.float32),
        "w_up": noise(arg_keys[10], (D, FF), D ** -0.5, 0.21875, ((1, 4),), jnp.float32),
        "w_down": noise(arg_keys[11], (FF, D), FF ** -0.5, 0.109375, ((0, 4),), jnp.float32),
        "grad_output": noise_with(arg_keys[12], (ITEMS, SLOTS, D), 1.0, 6.0, ((0, 8), (1, 4)), (0, 2, 8, 2.0), jnp.float32),
    }


@jax.custom_vjp
def low(v):
    return lax.optimization_barrier(v.astype(jnp.bfloat16)).astype(jnp.float32)

@jax.custom_vjp
def low_back(v):
    return v

def low_keep(v):
    return (low(v), None)

def low_pass(kept, grad):
    return (grad,)

def back_keep(v):
    return (v, None)

def back_low(kept, grad):
    return (low(grad),)
low.defvjp(low_keep, low_pass)
low_back.defvjp(back_keep, back_low)
EPSILON = 1e-05
HUGE = 1e+30

def precise(form, left, right):
    return jnp.einsum(form, left, right, precision=lax.Precision.HIGHEST)

def layer_norm(values, gain, bias):
    center = values - lax.optimization_barrier(jnp.mean(values, -1, keepdims=True))
    spread = lax.optimization_barrier(jnp.mean(center * center, -1, keepdims=True))
    return center * lax.rsqrt(spread + EPSILON) * gain + bias

def attend_item(operands):
    queries, keys_all, values_all, length = operands
    slot_count = queries.shape[0]
    scores = precise('qhe,khe->hqk', queries, keys_all) / math.sqrt(HD)
    query_pos = jnp.arange(slot_count)[:, None]
    key_pos = jnp.arange(slot_count)[None, :]
    allowed = (key_pos <= query_pos) & (key_pos < length)
    scores = jnp.where(allowed[None], scores, -HUGE)
    probs = jax.nn.softmax(scores, axis=-1)
    return precise('hqk,khe->qhe', probs, values_all).reshape(slot_count, HEADS * HD)

def reference(block_input, passes, pass_map, pass_table, gain_one, bias_one, w_qkv, w_out, gain_two, bias_two, w_up, w_down, grad_output):
    lengths = passes * BASE
    slot_pos = jnp.arange(SLOTS)
    live_rows = (slot_pos[None, :] < lengths[:, None]).astype(jnp.float32)[:, :, None]
    onehot = (pass_map[:, :, None] == jnp.arange(PASSES_MAX)[None, None, :]).astype(jnp.float32)

    def forward(inputs, table, gain_a, bias_a, qkv_weight, out_weight, gain_b, bias_b, up_weight, down_weight):
        start_rows = inputs + precise('isp,pd->isd', onehot, table)
        normed = layer_norm(start_rows, gain_a, bias_a)
        projected = precise('isd,dcf->iscf', normed, qkv_weight)
        head_shape = (ITEMS, SLOTS, HEADS, HD)
        queries = projected[:, :, 0].reshape(head_shape)
        keys_all = projected[:, :, 1].reshape(head_shape)
        values_all = projected[:, :, 2].reshape(head_shape)
        mixed = lax.map(jax.checkpoint(attend_item), (queries, keys_all, values_all, lengths))
        middle = start_rows + live_rows * precise('isf,fd->isd', mixed, out_weight)
        second = layer_norm(middle, gain_b, bias_b)
        hidden = jax.nn.gelu(precise('isd,df->isf', second, up_weight), approximate=True)
        return middle + live_rows * precise('isf,fd->isd', hidden, down_weight)
    outputs, back = jax.vjp(forward, block_input, pass_table, gain_one, bias_one, w_qkv, w_out, gain_two, bias_two, w_up, w_down)
    grads = back(grad_output)
    return (outputs, grads[0], grads[1], grads[2], grads[3], grads[4], grads[5], grads[6], grads[7], grads[8], grads[9])
```

```python
import math
import functools
import jax
import jax.numpy as jnp
from jax import lax
from jax.experimental import pallas as pl
from jax.experimental.pallas import tpu as pltpu
from jax.sharding import PartitionSpec as P

f32 = jnp.float32
bf16 = jnp.bfloat16
HD = 64
BASE = 256
PASSES_MAX = 5
EPSILON = 1e-05
HUGE = 1e30
QB = 256
HIGH = lax.Precision.HIGH
MESH = pl.DeviceIdType.MESH
NN = (((1,), (0,)), ((), ()))
NT = (((1,), (1,)), ((), ()))
TN = (((0,), (0,)), ((), ()))


def mm(left, right, dims=NN):
    return lax.dot_general(left, right, dims, precision=HIGH, preferred_element_type=f32)


def bdot(left, right, dims=NN):
    return lax.dot_general(left, right, dims, preferred_element_type=f32)


def halves(value):
    high = value.astype(bf16)
    return high, (value - high.astype(f32)).astype(bf16)


def rcopy(src, dst, send, recv, where):
    return pltpu.make_async_remote_copy(
        src_ref=src, dst_ref=dst, send_sem=send, recv_sem=recv, device_id=where, device_id_type=MESH
    )


def places():
    t = lax.axis_index("tensor")
    sib = t + 1 - 2 * (t % 2)
    yp = (t + 2) % 4
    far = (sib + 2) % 4
    return t, sib, yp, far


def greet(others):
    barrier = pltpu.get_barrier_semaphore()
    for other in others:
        pl.semaphore_signal(barrier, inc=1, device_id=other, device_id_type=MESH)
    pl.semaphore_wait(barrier, len(others))


def block(owner, rows, chunk=0, chunks=1):
    size = rows // chunks
    return pl.ds(pl.multiple_of(owner * rows + chunk * size, 8), size)


class Gather:
    def __init__(self, buf, send, recv, rows, chunks):
        t, sib, yp, far = places()
        self.own, self.yp, self.sib, self.far, self.rows, self.chunks = t, yp, sib, far, rows, chunks
        self.across, self.fwd = [], []
        mine = buf.at[block(t, rows)]
        self.side = rcopy(mine, mine, send.at[0], recv.at[0], {"tensor": sib})
        for k in range(chunks):
            part = buf.at[block(t, rows, k, chunks)]
            self.across.append(rcopy(part, part, send.at[1 + k], recv.at[1 + k], {"tensor": yp}))
            part = buf.at[block(yp, rows, k, chunks)]
            j = 1 + chunks + k
            self.fwd.append(rcopy(part, part, send.at[j], recv.at[j], {"tensor": sib}))

    def start(self):
        for c in self.across:
            c.start()
        self.side.start()

    def relay(self, k):
        self.across[k].wait_recv()
        self.fwd[k].start()

    def finish_sends(self):
        self.side.wait_send()
        for c in self.across + self.fwd:
            c.wait_send()


class Scatter:
    def __init__(self, part, own_in, pre_in, y_in, send, recv, rows, chunks):
        t, sib, yp, far = places()
        self.part, self.own_in, self.pre_in, self.y_in = part, own_in, pre_in, y_in
        self.rows, self.chunks, self.size = rows, chunks, rows // chunks
        self.t, self.sib, self.yp, self.far = t, sib, yp, far
        self.side = rcopy(part.at[block(sib, rows)], own_in, send.at[0], recv.at[0], {"tensor": sib})
        self.pre, self.across = [], []
        for k in range(chunks):
            here = pl.ds(k * self.size, self.size)
            self.pre.append(
                rcopy(part.at[block(far, rows, k, chunks)], pre_in.at[here], send.at[1 + k], recv.at[1 + k], {"tensor": sib})
            )
            j = 1 + chunks + k
            self.across.append(rcopy(pre_in.at[here], y_in.at[here], send.at[j], recv.at[j], {"tensor": yp}))

    def send_pre(self, k):
        self.pre[k].start()

    def send_across(self, k):
        self.pre[k].wait_recv()
        here = pl.ds(k * self.size, self.size)
        self.pre_in[here, :] = self.part[block(self.yp, self.rows, k, self.chunks), :] + self.pre_in[here, :]
        self.across[k].start()

    def send_side(self):
        self.side.start()

    def arrive(self):
        self.side.wait_recv()
        for c in self.across:
            c.wait_recv()

    def total(self, start, size):
        here = pl.ds(start, size)
        mine = pl.ds(pl.multiple_of(self.t * self.rows + start, 8), size)
        return self.part[mine, :] + self.own_in[here, :] + self.y_in[here, :]

    def finish_sends(self):
        self.side.wait_send()
        for c in self.pre + self.across:
            c.wait_send()


def slot_facts(start, passes_ref):
    count = passes_ref[0]
    slot = start + lax.broadcasted_iota(jnp.int32, (RS, 1), 0)
    which = jnp.zeros_like(slot)
    for r in range(1, PASSES_MAX + 1):
        which = jnp.where(count == r, slot % r, which)
    return which, jnp.where(slot < count * BASE, 1.0, 0.0)


def embed(x_ref, which, table_ref, here):
    rows = x_ref[here, :]
    added = jnp.zeros_like(rows)
    for p in range(PASSES_MAX):
        added = jnp.where(which == p, table_ref[pl.ds(p, 1), :], added)
    return rows + added


def norm_stats(values):
    center = values - jnp.mean(values, -1, keepdims=True)
    spread = jnp.mean(center * center, -1, keepdims=True)
    scale = lax.rsqrt(spread + EPSILON)
    return center * scale, scale


RS = 32


def over_rows(rows, body, size=RS):
    def step(i, carry):
        body(pl.multiple_of(i * size, size))
        return carry

    lax.fori_loop(0, rows // size, step, 0)


def cat_q(v):
    high = v.astype(bf16).astype(f32)
    low = v - high
    return jnp.concatenate([high, low, low, high], axis=1).astype(bf16)


def cat_k(v):
    high = v.astype(bf16).astype(f32)
    low = v - high
    return jnp.concatenate([high, low, high, low], axis=1).astype(bf16)


def fold(both):
    return both[:, :HD] + both[:, HD:]


def causal(s, size):
    row = lax.broadcasted_iota(jnp.int32, (QB, QB), 0)
    col = lax.broadcasted_iota(jnp.int32, (QB, QB), 1)
    last = jnp.where(col <= row, s[:, size - QB :], -HUGE)
    return last if size == QB else jnp.concatenate([s[:, : size - QB], last], axis=1)


def add_eight(ref, row, value):
    total = value[0:8, :]
    for k in range(1, value.shape[0] // 8):
        total = total + value[8 * k : 8 * k + 8, :]
    ref[pl.ds(row, 8), :] = ref[pl.ds(row, 8), :] + total


def forward_kernel(
    dims, passes, x, table, vecs, go, wq_h, wo_h,
    a_o, qc_o, kc_o, vc_o, o_o, lse_o, h1_o, c_o, dz_o,
    A, DZ, QC, KC, VC, OH, O, LSE, PT, OWN, PRE, YIN, WQ, WO,
    s1, r1, s2, r2, s3, r3, ls,
):
    rows, slots, feats, heads, chunks = dims
    t, sib, yp, far = places()
    mine0 = t * rows
    loads = [pltpu.make_async_copy(wq_h.at[c], WQ.at[c], ls.at[c]) for c in range(3)]
    loads.append(pltpu.make_async_copy(wo_h, WO, ls.at[3]))
    for c in loads:
        c.start()

    def begin_rows(r):
        here = pl.ds(r, RS)
        which, live = slot_facts(mine0 + r, passes)
        h0 = embed(x, which, table, here)
        h1_o[here, :] = h0
        xhat, _ = norm_stats(h0)
        mine = pl.ds(pl.multiple_of(mine0 + r, RS), RS)
        A[mine, :] = xhat * vecs[0:1, :] + vecs[1:2, :]
        DZ[mine, :] = live * go[here, :]

    over_rows(rows, begin_rows)
    greet([{"tensor": sib}, {"tensor": yp}])
    ga = Gather(A, s1, r1, rows, chunks)
    gz = Gather(DZ, s2, r2, rows, chunks)
    ga.start()
    for c in loads:
        c.wait()

    def project(owner):
        here = block(owner, rows)
        for c, (ref, cat) in enumerate(((QC, cat_q), (KC, cat_k), (VC, cat_k))):
            pr = mm(A[here, :], WQ[c])
            if c == 0:
                pr = pr * (1.0 / math.sqrt(HD))
            for h in range(heads):
                ref[h, here, :] = cat(pr[:, h * HD : (h + 1) * HD])

    project(t)
    ga.side.wait_recv()
    project(sib)
    for k in range(chunks):
        ga.relay(k)
    gz.start()
    project(yp)
    for k in range(chunks):
        ga.fwd[k].wait_recv()
    project(far)
    outs = [
        pltpu.make_async_copy(A, a_o, ls.at[4]),
        pltpu.make_async_copy(QC, qc_o, ls.at[5]),
        pltpu.make_async_copy(KC, kc_o, ls.at[6]),
        pltpu.make_async_copy(VC, vc_o, ls.at[7]),
    ]
    for c in outs:
        c.start()
    lane = lax.broadcasted_iota(jnp.int32, (QB, 128), 1)
    for i in reversed(range(slots // QB)):
        q_rows = pl.ds(i * QB, QB)
        size = (i + 1) * QB

        def one_head(h, carry):
            s = causal(bdot(QC[h, q_rows, :], KC[h, pl.ds(0, size), :], NT), size)
            top = jnp.max(s, -1, keepdims=True)
            p = jnp.exp(s - top)
            total = jnp.sum(p, -1, keepdims=True)
            ph, pw = halves(p)
            values = VC[h, pl.ds(0, size), 0 : 2 * HD]
            OH[h, :, :] = fold(bdot(ph, values) + bdot(pw, values)) / total
            old = LSE[q_rows, :]
            LSE[q_rows, :] = jnp.where(lane == h, top + jnp.log(total), old)
            return carry

        LSE[q_rows, :] = jnp.zeros((QB, 128), f32)
        lax.fori_loop(0, heads, one_head, 0)
        o = jnp.concatenate([OH[h] for h in range(heads)], axis=1)
        O[q_rows, :] = o
        PT[q_rows, :] = mm(o, WO[...])
    rs = Scatter(PT, OWN, PRE, YIN, s3, r3, rows, chunks)
    for k in range(chunks):
        rs.send_pre(k)
    for k in range(chunks):
        rs.send_across(k)
    rs.send_side()
    gz.side.wait_recv()
    for k in range(chunks):
        gz.relay(k)
    more = [pltpu.make_async_copy(O, o_o, ls.at[8]), pltpu.make_async_copy(LSE, lse_o, ls.at[9])]
    for c in more:
        c.start()
    for k in range(chunks):
        gz.fwd[k].wait_recv()
    dz_copy = pltpu.make_async_copy(DZ, dz_o, ls.at[10])
    dz_copy.start()
    rs.arrive()

    def end_rows(r):
        here = pl.ds(r, RS)
        _, live = slot_facts(mine0 + r, passes)
        h1 = h1_o[here, :] + live * rs.total(r, RS)
        h1_o[here, :] = h1
        xhat, _ = norm_stats(h1)
        c_o[here, :] = xhat * vecs[2:3, :] + vecs[3:4, :]

    over_rows(rows, end_rows)
    for c in outs + more + [dz_copy]:
        c.wait()
    ga.finish_sends()
    gz.finish_sends()
    rs.finish_sends()


def struct(*shape):
    return jax.ShapeDtypeStruct(shape, f32)


def vm(*shape):
    return pltpu.VMEM(shape, f32)


def vb(*shape):
    return pltpu.VMEM(shape, bf16)


def pairs(count, *numbers):
    return [pltpu.SemaphoreType.DMA((n,)) for n in numbers for _ in range(count)]


IN_VMEM = pl.BlockSpec(memory_space=pltpu.VMEM)
IN_SMEM = pl.BlockSpec(memory_space=pltpu.SMEM)
IN_HBM = pl.BlockSpec(memory_space=pl.ANY)
CHUNKS = 2


def params(number):
    return pltpu.CompilerParams(collective_id=number, has_side_effects=True, vmem_limit_bytes=63 << 20)


def forward_call(passes, x, table, vecs, go, wq, wo, slots):
    rows, feats = x.shape
    local = wq.shape[2]
    heads = local // HD
    cat = jax.ShapeDtypeStruct((heads, slots, 4 * HD), bf16)
    ng = 1 + 2 * CHUNKS
    return pl.pallas_call(
        functools.partial(forward_kernel, (rows, slots, feats, heads, CHUNKS)),
        out_shape=(
            struct(slots, feats), cat, cat, cat, struct(slots, local), struct(slots, 128),
            struct(rows, feats), struct(rows, feats), struct(slots, feats),
        ),
        in_specs=[IN_SMEM] + [IN_VMEM] * 4 + [IN_HBM] * 2,
        out_specs=(IN_HBM,) * 6 + (IN_VMEM, IN_VMEM, IN_HBM),
        scratch_shapes=[
            vm(slots, feats), vm(slots, feats),
            vb(heads, slots, 4 * HD), vb(heads, slots, 4 * HD), vb(heads, slots, 4 * HD),
            vm(heads, QB, HD), vm(slots, local), vm(slots, 128), vm(slots, feats),
            vm(rows, feats), vm(rows, feats), vm(rows, feats),
            vm(3, feats, local), vm(local, feats),
        ] + pairs(2, ng, ng, ng) + pairs(1, 11),
        compiler_params=params(1),
        name="forward_part",
    )(passes, x, table, vecs, go, wq, wo)


def gelu_both(u):
    k = math.sqrt(2.0 / math.pi)
    square = u * u
    th = jnp.tanh(k * (u * (1.0 + 0.044715 * square)))
    half = 0.5 * (1.0 + th)
    slope = half + (0.5 * k) * u * (1.0 - th * th) * (1.0 + (3.0 * 0.044715) * square)
    return u * half, slope


def middle_kernel(
    dims, h1, go, vecs, c_h, dz_h, wu_h, wd_h,
    dh1_o, vec_o, zp_o, gd_o, gu_o,
    C, DZ, ACT, DU, PT, OWN, PRE, YIN, WU, WD, GD, GU,
    s1, r1, s2, r2, ls,
):
    rows, slots, feats, chunks = dims
    t, sib, yp, far = places()
    first = pltpu.make_async_copy(c_h, C.at[block(t, rows)], ls.at[0])
    loads = [
        pltpu.make_async_copy(wd_h, WD, ls.at[1]),
        pltpu.make_async_copy(dz_h, DZ, ls.at[2]),
        pltpu.make_async_copy(wu_h, WU, ls.at[3]),
    ]
    first.start()
    for c in loads:
        c.start()
    greet([{"tensor": sib}, {"tensor": yp}])
    first.wait()
    gc = Gather(C, s1, r1, rows, chunks)
    gc.start()
    for c in loads:
        c.wait()

    def open_block(i, carry):
        here = block(i, rows)
        DU[here, :] = mm(DZ[here, :], WD[...], NT)
        return carry

    lax.fori_loop(0, slots // rows, open_block, 0)

    def work(here):
        act, slope = gelu_both(mm(C[here, :], WU[...]))
        ACT[here, :] = act
        du = DU[here, :] * slope
        DU[here, :] = du
        PT[here, :] = mm(du, WU[...], NT)

    rs = Scatter(PT, OWN, PRE, YIN, s2, r2, rows, chunks)
    size = rows // chunks

    def whole(owner):
        def step(k, carry):
            work(pl.ds(pl.multiple_of(owner * rows + k * size, 8), size))
            return carry

        lax.fori_loop(0, chunks, step, 0)

    whole(t)
    gc.side.wait_recv()
    whole(sib)
    rs.send_side()
    for k in range(chunks):
        gc.relay(k)
        gc.fwd[k].wait_recv()
        work(block(far, rows, k, chunks))
        rs.send_pre(k)
        work(block(yp, rows, k, chunks))
        rs.send_across(k)

    GU[...] = mm(C[...], DU[...], TN)
    gu_copy = pltpu.make_async_copy(GU, gu_o, ls.at[4])
    gu_copy.start()
    GD[...] = mm(DZ[...], ACT[...], TN)
    gd_copy = pltpu.make_async_copy(GD, gd_o, ls.at[5])
    gd_copy.start()

    def down(i, carry):
        here = block(i, rows)
        DZ[here, :] = mm(ACT[here, :], WD[...])
        return carry

    lax.fori_loop(0, slots // rows, down, 0)
    zp_copy = pltpu.make_async_copy(DZ, zp_o, ls.at[6])
    zp_copy.start()
    vec_o[...] = jnp.zeros_like(vec_o)
    rs.arrive()

    def end_rows(r):
        here = pl.ds(r, RS)
        dc = rs.total(r, RS)
        xhat, scale = norm_stats(h1[here, :])
        add_eight(vec_o, 0, dc * xhat)
        add_eight(vec_o, 8, dc)
        e = dc * vecs[2:3, :]
        inner = e - jnp.mean(e, -1, keepdims=True) - xhat * jnp.mean(e * xhat, -1, keepdims=True)
        dh1_o[here, :] = go[here, :] + inner * scale

    over_rows(rows, end_rows)
    for c in (gu_copy, gd_copy, zp_copy):
        c.wait()
    gc.finish_sends()
    rs.finish_sends()


def middle_call(h1, go, vecs, c, dz, wu, wd):
    rows, feats = h1.shape
    slots = dz.shape[0]
    hidden = wu.shape[1]
    ng = 1 + 2 * CHUNKS
    return pl.pallas_call(
        functools.partial(middle_kernel, (rows, slots, feats, CHUNKS)),
        out_shape=(struct(rows, feats), struct(16, feats), struct(slots, feats), struct(feats, hidden), struct(feats, hidden)),
        in_specs=[IN_VMEM] * 3 + [IN_HBM] * 4,
        out_specs=(IN_VMEM, IN_VMEM, IN_HBM, IN_HBM, IN_HBM),
        scratch_shapes=[
            vm(slots, feats), vm(slots, feats), vm(slots, hidden), vm(slots, hidden), vm(slots, feats),
            vm(rows, feats), vm(rows, feats), vm(rows, feats),
            vm(feats, hidden), vm(hidden, feats), vm(feats, hidden), vm(feats, hidden),
        ] + pairs(2, ng, ng) + pairs(1, 7),
        compiler_params=params(2),
        name="middle_part",
    )(h1, go, vecs, c, dz, wu, wd)


class Halve:
    def __init__(self, source, keep, in_one, in_two, in_three, send, recv, base):
        d = lax.axis_index("dp")
        self.low, self.mid, self.top = d % 2, (d // 2) % 2, d // 4
        self.keep, self.ins = keep, (in_one, in_two, in_three)
        p1 = {"dp": d + 1 - 2 * self.low}
        p2 = {"dp": d + 2 - 4 * self.mid}
        p4 = {"dp": (d + 4) % 8}
        self.one = [
            rcopy(source.at[j, 1 - self.low], in_one.at[j], send.at[base + j], recv.at[base + j], p1) for j in range(4)
        ]
        self.two = [
            rcopy(keep.at[2 * j + 1 - self.mid], in_two.at[j], send.at[base + 4 + j], recv.at[base + 4 + j], p2) for j in range(2)
        ]
        self.three = rcopy(keep.at[2 * (1 - self.top) + self.mid], in_three, send.at[base + 6], recv.at[base + 6], p4)

    def start_one(self):
        for c in self.one:
            c.start()

    def take_one(self):
        for c in self.one:
            c.wait_recv()
        self.keep[...] = self.keep[...] + self.ins[0][...]
        for c in self.two:
            c.start()

    def take_two(self):
        for j in range(2):
            self.two[j].wait_recv()
            at = 2 * j + self.mid
            self.keep[at] = self.keep[at] + self.ins[1][j]
        self.three.start()

    def take_three(self, out):
        self.three.wait_recv()
        out[...] = self.keep[2 * self.top + self.mid] + self.ins[2][...]

    def finish_sends(self):
        for c in self.one + self.two + [self.three]:
            c.wait_send()


def backward_kernel(dims, *refs):
    rows, slots, feats, heads, chunks, halving = dims
    refs = list(refs)

    def take(n):
        out = refs[:n]
        del refs[:n]
        return out

    passes, x, table, vecs, h1, dh1, vec2 = take(7)
    qc_h, kc_h, vc_h, o_h, lse_h, a_h, zp_h, wq_h, wo_h = take(9)
    if halving:
        gd_h, gu_h = take(2)
    out_o, gi_o, vec_o, gt_o, gq_o = take(5)
    if halving:
        gd_o, gu_o = take(2)
    QC, KC, VC, DOC, LSE, DELTA, DATT, DQ, DK, DV, DP = take(11)
    OWN, PRE, YIN, ZP, ZOWN, ZPRE, ZYIN, WQ, WO, ACC, VB, VIN = take(12)
    if halving:
        GT, GQ, KD, KU, KT, KQ, D1, D2, D3, U1, U2, U3, T1, T2, T3, Q1, Q2, Q3 = take(18)
    s1, r1, s2, r2, s3, r3, sv, rv, ls = take(9)
    if halving:
        sh, rh = take(2)
    O = DP.at[0]
    t, sib, yp, far = places()
    mine0 = t * rows
    loads = [
        pltpu.make_async_copy(src, dst, ls.at[n])
        for n, (src, dst) in enumerate(
            ((wo_h, WO), (o_h, DP.at[0]), (zp_h, ZP), (qc_h, QC), (kc_h, KC), (vc_h, VC), (lse_h, LSE))
        )
    ]
    loads += [pltpu.make_async_copy(wq_h.at[c], WQ.at[c], ls.at[7 + c]) for c in range(3)]
    if halving:
        d = lax.axis_index("dp")
        low = d % 2
        mine_d = [pltpu.make_async_copy(gd_h.at[j, low], KD.at[j], ls.at[10 + j]) for j in range(4)]
        mine_u = [pltpu.make_async_copy(gu_h.at[j, low], KU.at[j], ls.at[14 + j]) for j in range(4)]
        loads += mine_d + mine_u
    for c in loads:
        c.start()

    def begin_rows(r):
        here = pl.ds(r, RS)
        _, live = slot_facts(mine0 + r, passes)
        DATT[pl.ds(pl.multiple_of(mine0 + r, RS), RS), :] = live * dh1[here, :]

    over_rows(rows, begin_rows)
    others = [{"tensor": sib}, {"tensor": yp}]
    if halving:
        dp_peers = [{"dp": d + 1 - 2 * low}, {"dp": d + 2 - 4 * ((d // 2) % 2)}, {"dp": (d + 4) % 8}]
        others = others + dp_peers
    greet(others)
    gt = Gather(DATT, s1, r1, rows, chunks)
    gt.start()
    if halving:
        hu = Halve(gu_h, KU, U1, U2, U3, sh, rh, 0)
        hd = Halve(gd_h, KD, D1, D2, D3, sh, rh, 7)
        hu.start_one()
        hd.start_one()
    rz = Scatter(ZP, ZOWN, ZPRE, ZYIN, s2, r2, rows, chunks)
    loads[2].wait()
    for k in range(chunks):
        rz.send_pre(k)
    rz.send_side()
    loads[0].wait()
    loads[1].wait()
    lane = lax.broadcasted_iota(jnp.int32, (rows, 128), 1)

    def mixed_grad(owner):
        here = block(owner, rows)
        do = mm(DATT[here, :], WO[...], NT)
        prod = do * O[here, :]
        delta = jnp.zeros((rows, 128), f32)
        for h in range(heads):
            cols = slice(h * HD, (h + 1) * HD)
            DOC[h, here, :] = cat_q(do[:, cols])
            delta = jnp.where(lane == h, jnp.sum(prod[:, cols], -1, keepdims=True), delta)
        DELTA[here, :] = delta

    mixed_grad(t)
    gt.side.wait_recv()
    mixed_grad(sib)
    for k in range(chunks):
        gt.relay(k)
    for k in range(chunks):
        rz.send_across(k)
    mixed_grad(yp)
    for k in range(chunks):
        gt.fwd[k].wait_recv()
    mixed_grad(far)
    grad_out = mm(DATT[...], O[...], TN)
    if halving:
        GT[...] = grad_out.reshape(GT.shape)
    else:
        gt_o[...] = grad_out
    for c in loads[3:]:
        c.wait()
    if halving:
        hu.take_one()
        ht = Halve(GT, KT, T1, T2, T3, sh, rh, 14)
        KT[...] = GT[:, low]
        ht.start_one()
        hd.take_one()
    gt.finish_sends()
    lane_q = lax.broadcasted_iota(jnp.int32, (QB, 128), 1)
    blocks = slots // QB
    for i in reversed(range(blocks)):
        q_rows = pl.ds(i * QB, QB)
        size = (i + 1) * QB
        k_rows = pl.ds(0, size)

        def one_head(h, carry):
            q, do = QC[h, q_rows, :], DOC[h, q_rows, :]
            pick = lane_q == h
            lse = jnp.sum(jnp.where(pick, LSE[q_rows, :], 0.0), -1, keepdims=True)
            delta = jnp.sum(jnp.where(pick, DELTA[q_rows, :], 0.0), -1, keepdims=True)
            s = causal(bdot(q, KC[h, k_rows, :], NT), size)
            p = jnp.exp(s - lse)
            ds = p * (bdot(do, VC[h, k_rows, :], NT) - delta)
            ph, pw = halves(p)
            dsh, dsw = halves(ds)
            do2, q2 = do[:, : 2 * HD], q[:, : 2 * HD]
            dv = bdot(ph, do2, TN) + bdot(pw, do2, TN)
            dk = bdot(dsh, q2, TN) + bdot(dsw, q2, TN)
            keys = KC[h, k_rows, 0 : 2 * HD]
            DQ[h, :, :] = bdot(dsh, keys) + bdot(dsw, keys)
            if i == blocks - 1:
                DV[h, :, :] = dv
                DK[h, :, :] = dk
            else:
                DV[h, k_rows, :] = DV[h, k_rows, :] + dv
                DK[h, k_rows, :] = DK[h, k_rows, :] + dk
            return carry

        lax.fori_loop(0, heads, one_head, 0)
        if halving and i == blocks - 1:
            hu.take_two()
            ht.take_one()
            hd.take_two()
        if halving and i == blocks - 3:
            ht.take_two()
            hu.take_three(gu_o)
            hd.take_three(gd_o)
        total = None
        for c, (ref, factor) in enumerate(((DQ, 1.0 / math.sqrt(HD)), (DK, None), (DV, None))):
            at = pl.ds(0, QB) if c == 0 else q_rows
            part = jnp.concatenate([fold(ref[h, at, :]) for h in range(heads)], axis=1)
            if factor is not None:
                part = part * factor
            DP[c, q_rows, :] = part
            term = mm(part, WQ[c], NT)
            total = term if total is None else total + term
        DATT[q_rows, :] = total
        if i == 1:
            rz.arrive()

            def out_rows(r):
                here = pl.ds(r, RS)
                _, live = slot_facts(mine0 + r, passes)
                out_o[here, :] = h1[here, :] + live * rz.total(r, RS)

            over_rows(rows, out_rows)
            rz.finish_sends()
            a_copy = pltpu.make_async_copy(a_h, ZP, ls.at[18])
            a_copy.start()
    rd = Scatter(DATT, OWN, PRE, YIN, s3, r3, rows, chunks)
    for k in range(chunks):
        rd.send_pre(k)
    a_copy.wait()

    def grad_w(c):
        full = mm(ZP[...], DP[c], TN)
        if not halving:
            gq_o[c] = full
            return None
        GQ[c] = full.reshape(GQ.shape[1:])
        KQ[c] = GQ[c, :, low]
        hq = Halve(GQ.at[c], KQ.at[c], Q1.at[c], Q2.at[c], Q3.at[c], sh, rh, 21 + 7 * c)
        hq.start_one()
        return hq

    hq = [grad_w(0)]
    for k in range(chunks):
        rd.send_across(k)
    rd.send_side()
    hq.append(grad_w(1))
    hq.append(grad_w(2))
    if halving:
        hq[0].take_one()
        ht.take_three(gt_o)
        hq[1].take_one()
        hq[0].take_two()
        hq[2].take_one()
        hq[1].take_two()
    ACC[...] = jnp.zeros_like(ACC)
    rd.arrive()

    def end_rows(r):
        here = pl.ds(r, RS)
        which, _ = slot_facts(mine0 + r, passes)
        xhat, scale = norm_stats(embed(x, which, table, here))
        da = rd.total(r, RS)
        add_eight(ACC, 0, da * xhat)
        add_eight(ACC, 8, da)
        e = da * vecs[0:1, :]
        inner = e - jnp.mean(e, -1, keepdims=True) - xhat * jnp.mean(e * xhat, -1, keepdims=True)
        gi = dh1[here, :] + inner * scale
        gi_o[here, :] = gi
        for p in range(PASSES_MAX):
            add_eight(ACC, 16 + 8 * p, jnp.where(which == p, gi, 0.0))

    over_rows(rows, end_rows)
    VB[0] = jnp.zeros_like(VB[0])
    for n in range(2):
        VB[0, pl.ds(n, 1), :] = jnp.sum(ACC[8 * n : 8 * n + 8, :], 0, keepdims=True)
        VB[0, pl.ds(2 + n, 1), :] = jnp.sum(vec2[8 * n : 8 * n + 8, :], 0, keepdims=True)
    for p in range(PASSES_MAX):
        VB[0, pl.ds(4 + p, 1), :] = jnp.sum(ACC[16 + 8 * p : 24 + 8 * p, :], 0, keepdims=True)
    rounds = []
    for n, other in enumerate(others):
        c = rcopy(VB.at[n], VIN.at[n], sv.at[n], rv.at[n], other)
        c.start()
        if halving and n == 1:
            hq[0].take_three(gq_o.at[0])
        if halving and n == 2:
            hq[2].take_two()
        c.wait_recv()
        VB[n + 1] = VB[n] + VIN[n]
        rounds.append(c)
    vec_o[...] = VB[len(others)]
    if halving:
        hq[1].take_three(gq_o.at[1])
        hq[2].take_three(gq_o.at[2])
        for h in [hu, hd, ht] + hq:
            h.finish_sends()
    for c in rounds:
        c.wait_send()
    rd.finish_sends()


def backward_call(passes, x, table, vecs, h1, dh1, vec2, qc, kc, vc, o, lse, a, zp, wq, wo, gd, gu, halving):
    rows, feats = x.shape
    slots, local = o.shape
    heads = local // HD
    hidden = gd.shape[1]
    ng = 1 + 2 * CHUNKS
    ends = 5 if halving else 2
    share = feats // 8
    cat = vb(heads, slots, 4 * HD)
    wide = vm(heads, slots, 2 * HD)
    outs = [struct(rows, feats), struct(rows, feats), struct(16, feats)]
    args = [passes, x, table, vecs, h1, dh1, vec2, qc, kc, vc, o, lse, a, zp, wq, wo]
    scratch = [
        cat, cat, cat, cat, vm(slots, 128), vm(slots, 128), vm(slots, feats), vm(heads, QB, 2 * HD), wide, wide, vm(3, slots, local),
        vm(rows, feats), vm(rows, feats), vm(rows, feats), vm(slots, feats), vm(rows, feats), vm(rows, feats), vm(rows, feats),
        vm(3, feats, local), vm(local, feats), vm(16 + 8 * PASSES_MAX, feats), vm(ends + 1, 16, feats), vm(ends, 16, feats),
    ]
    sems = pairs(2, ng, ng, ng, ends) + pairs(1, 19)
    if halving:
        outs += [struct(share, local), struct(3, share, local), struct(share, hidden), struct(share, hidden)]
        args += [gd.reshape(4, 2, share, hidden), gu.reshape(4, 2, share, hidden)]
        scratch += [vm(4, 2, share, local), vm(3, 4, 2, share, local)]
        scratch += [vm(4, share, hidden), vm(4, share, hidden), vm(4, share, local), vm(3, 4, share, local)]
        for width in (hidden, hidden, local):
            scratch += [vm(4, share, width), vm(2, share, width), vm(share, width)]
        scratch += [vm(3, 4, share, local), vm(3, 2, share, local), vm(3, share, local)]
        sems += pairs(2, 42)
    else:
        outs += [struct(feats, local), struct(3, feats, local)]
    return pl.pallas_call(
        functools.partial(backward_kernel, (rows, slots, feats, heads, CHUNKS, halving)),
        out_shape=tuple(outs),
        in_specs=[IN_SMEM] + [IN_VMEM] * 6 + [IN_HBM] * (len(args) - 7),
        out_specs=(IN_VMEM,) * len(outs),
        scratch_shapes=scratch + sems,
        compiler_params=params(3),
        name="backward_part",
    )(*args)


def per_device(
    block_input, passes, pass_map, pass_table, gain_one, bias_one, w_qkv, w_out, gain_two, bias_two, w_up, w_down, grad_output
):
    x, go = block_input[0], grad_output[0]
    rows, feats = x.shape
    slots = rows * lax.axis_size("tensor")
    ways = lax.axis_size("dp")
    halving = ways == 8
    vecs = jnp.stack([gain_one, bias_one, gain_two, bias_two])
    w_qkv = jnp.swapaxes(w_qkv, 0, 1)
    a, qc, kc, vc, o, lse, h1, c, dz = forward_call(passes, x, pass_table, vecs, go, w_qkv, w_out, slots)
    dh1, vec2, zp, gd, gu = middle_call(h1, go, vecs, c, dz, w_up, w_down)
    got = backward_call(passes, x, pass_table, vecs, h1, dh1, vec2, qc, kc, vc, o, lse, a, zp, w_qkv, w_out, gd, gu, halving)
    out, gi, vec, gt, gq = got[:5]
    gq = jnp.swapaxes(gq, 0, 1)
    if halving:
        gd, gu = got[5:]
        share = feats // ways
        part = lax.dynamic_slice_in_dim(vec, lax.axis_index("dp") * share, share, 1)
    else:
        gt, gq, gu, gd = (lax.psum_scatter(v, "dp", scatter_dimension=0, tiled=True) for v in (gt, gq, gu, gd))
        part = lax.psum_scatter(vec, "dp", scatter_dimension=1, tiled=True)
    return (
        out[None], gi[None], part[4 : 4 + PASSES_MAX], part[0], part[1], gq, gt.T, part[2], part[3], gu, gd.T,
    )


def solution(mesh):
    placed = (
        P("dp", "tensor", None), P("dp"), P("dp", "tensor"), P(), P(), P(), P(None, None, "tensor"), P("tensor", None),
        P(), P(), P(None, "tensor"), P("tensor", None), P("dp", "tensor", None),
    )
    return jax.shard_map(
        per_device,
        mesh=mesh,
        in_specs=placed,
        out_specs=(
            P("dp", "tensor", None), P("dp", "tensor", None), P(None, "dp"), P("dp"), P("dp"), P("dp", None, "tensor"),
            P("tensor", "dp"), P("dp"), P("dp"), P("dp", "tensor"), P("tensor", "dp"),
        ),
        check_vma=False,
    )
```

```python
import math
import functools
import jax
import jax.numpy as jnp
from jax import lax
from jax.experimental import pallas as pl
from jax.experimental.pallas import tpu as pltpu
from jax.sharding import PartitionSpec as P

f32 = jnp.float32
bf16 = jnp.bfloat16
HD = 64
BASE = 256
PASSES_MAX = 5
EPSILON = 1e-05
HUGE = 1e30
QB = 256
HIGH = lax.Precision.HIGH
MESH = pl.DeviceIdType.MESH
NN = (((1,), (0,)), ((), ()))
NT = (((1,), (1,)), ((), ()))
TN = (((0,), (0,)), ((), ()))


def mm(left, right, dims=NN):
    return lax.dot_general(left, right, dims, precision=HIGH, preferred_element_type=f32)


def bdot(left, right, dims=NN):
    return lax.dot_general(left, right, dims, preferred_element_type=f32)


def halves(value):
    high = value.astype(bf16)
    return high, (value - high.astype(f32)).astype(bf16)


def rcopy(src, dst, send, recv, where):
    return pltpu.make_async_remote_copy(
        src_ref=src, dst_ref=dst, send_sem=send, recv_sem=recv, device_id=where, device_id_type=MESH
    )


def places():
    t = lax.axis_index("tensor")
    sib = t + 1 - 2 * (t % 2)
    yp = (t + 2) % 4
    far = (sib + 2) % 4
    return t, sib, yp, far


def greet(others):
    barrier = pltpu.get_barrier_semaphore()
    for other in others:
        pl.semaphore_signal(barrier, inc=1, device_id=other, device_id_type=MESH)
    pl.semaphore_wait(barrier, len(others))


def order_of(n, owners):
    out = owners[0]
    for k in range(1, len(owners)):
        here = (n + len(owners) - k) // len(owners) - (n + len(owners) - k - 1) // len(owners)
        out = out + here * (owners[k] - owners[0])
    return out


def block(owner, rows, chunk=0, chunks=1):
    size = rows // chunks
    return pl.ds(pl.multiple_of(owner * rows + chunk * size, 8), size)


class Gather:
    def __init__(self, buf, send, recv, rows, chunks):
        t, sib, yp, far = places()
        self.own, self.yp, self.sib, self.far, self.rows, self.chunks = t, yp, sib, far, rows, chunks
        self.across, self.fwd = [], []
        mine = buf.at[block(t, rows)]
        self.side = rcopy(mine, mine, send.at[0], recv.at[0], {"tensor": sib})
        for k in range(chunks):
            part = buf.at[block(t, rows, k, chunks)]
            self.across.append(rcopy(part, part, send.at[1 + k], recv.at[1 + k], {"tensor": yp}))
            part = buf.at[block(yp, rows, k, chunks)]
            j = 1 + chunks + k
            self.fwd.append(rcopy(part, part, send.at[j], recv.at[j], {"tensor": sib}))

    def start(self):
        for c in self.across:
            c.start()
        self.side.start()

    def relay(self, k):
        self.across[k].wait_recv()
        self.fwd[k].start()

    def finish_sends(self):
        self.side.wait_send()
        for c in self.across + self.fwd:
            c.wait_send()


class Scatter:
    def __init__(self, part, own_in, pre_in, y_in, send, recv, rows, chunks):
        t, sib, yp, far = places()
        self.part, self.own_in, self.pre_in, self.y_in = part, own_in, pre_in, y_in
        self.rows, self.chunks, self.size = rows, chunks, rows // chunks
        self.t, self.sib, self.yp, self.far = t, sib, yp, far
        self.side = rcopy(part.at[block(sib, rows)], own_in, send.at[0], recv.at[0], {"tensor": sib})
        self.pre, self.across = [], []
        for k in range(chunks):
            here = pl.ds(k * self.size, self.size)
            self.pre.append(
                rcopy(part.at[block(far, rows, k, chunks)], pre_in.at[here], send.at[1 + k], recv.at[1 + k], {"tensor": sib})
            )
            j = 1 + chunks + k
            self.across.append(rcopy(pre_in.at[here], y_in.at[here], send.at[j], recv.at[j], {"tensor": yp}))

    def send_pre(self, k):
        self.pre[k].start()

    def send_across(self, k):
        self.pre[k].wait_recv()
        here = pl.ds(k * self.size, self.size)
        self.pre_in[here, :] = self.part[block(self.yp, self.rows, k, self.chunks), :] + self.pre_in[here, :]
        self.across[k].start()

    def send_side(self):
        self.side.start()

    def arrive(self):
        self.side.wait_recv()
        for c in self.across:
            c.wait_recv()

    def total(self, start, size):
        here = pl.ds(start, size)
        mine = pl.ds(pl.multiple_of(self.t * self.rows + start, 8), size)
        return self.part[mine, :] + self.own_in[here, :] + self.y_in[here, :]

    def finish_sends(self):
        self.side.wait_send()
        for c in self.pre + self.across:
            c.wait_send()


def slot_facts(start, passes_ref):
    count = passes_ref[0]
    slot = start + lax.broadcasted_iota(jnp.int32, (RS, 1), 0)
    which = jnp.zeros_like(slot)
    for r in range(1, PASSES_MAX + 1):
        which = jnp.where(count == r, slot % r, which)
    return which, jnp.where(slot < count * BASE, 1.0, 0.0)


def embed(x_ref, which, table_ref, here):
    rows = x_ref[here, :]
    added = jnp.zeros_like(rows)
    for p in range(PASSES_MAX):
        added = jnp.where(which == p, table_ref[pl.ds(p, 1), :], added)
    return rows + added


def norm_stats(values):
    center = values - jnp.mean(values, -1, keepdims=True)
    spread = jnp.mean(center * center, -1, keepdims=True)
    scale = lax.rsqrt(spread + EPSILON)
    return center * scale, scale


RS = 32


def over_rows(rows, body, size=RS):
    def step(i, carry):
        body(pl.multiple_of(i * size, size))
        return carry

    lax.fori_loop(0, rows // size, step, 0)


def cat_q(v):
    high = v.astype(bf16).astype(f32)
    low = v - high
    return jnp.concatenate([high, low, low, high], axis=1).astype(bf16)


def cat_k(v):
    high = v.astype(bf16).astype(f32)
    low = v - high
    return jnp.concatenate([high, low, high, low], axis=1).astype(bf16)


def fold(both):
    return both[:, :HD] + both[:, HD:]


def causal(s, size):
    row = lax.broadcasted_iota(jnp.int32, (QB, QB), 0)
    col = lax.broadcasted_iota(jnp.int32, (QB, QB), 1)
    last = jnp.where(col <= row, s[:, size - QB :], -HUGE)
    return last if size == QB else jnp.concatenate([s[:, : size - QB], last], axis=1)


def add_eight(ref, row, value):
    total = value[0:8, :]
    for k in range(1, value.shape[0] // 8):
        total = total + value[8 * k : 8 * k + 8, :]
    ref[pl.ds(row, 8), :] = ref[pl.ds(row, 8), :] + total


def row_of(ref):
    return ref[...].reshape(1, ref.shape[0])


def forward_kernel(
    dims, passes, x, table, g1, b1, g2, b2, go, w_h, wo_h,
    a_o, qc_o, kc_o, vc_o, o_o, lse_o, wq_o, h1_o, c_o, dz_o,
    A, DZ, QC, KC, VC, O, LSE, TOP, SUM, OT, PT, OWN, PRE, YIN, W3, WQ, WO,
    s1, r1, s2, r2, s3, r3, ls,
):
    rows, slots, feats, heads, chunks = dims
    t, sib, yp, far = places()
    mine0 = t * rows
    loads = [pltpu.make_async_copy(w_h, W3, ls.at[0]), pltpu.make_async_copy(wo_h, WO, ls.at[1])]
    for c in loads:
        c.start()
    gain, bias = row_of(g1), row_of(b1)

    def begin_rows(r):
        here = pl.ds(r, RS)
        which, live = slot_facts(mine0 + r, passes)
        h0 = embed(x, which, table, here)
        h1_o[here, :] = h0
        xhat, _ = norm_stats(h0)
        mine = pl.ds(pl.multiple_of(mine0 + r, RS), RS)
        A[mine, :] = xhat * gain + bias
        DZ[mine, :] = live * go[here, :]

    over_rows(rows, begin_rows)
    greet([{"tensor": sib}, {"tensor": yp}])
    ga = Gather(A, s1, r1, rows, chunks)
    gz = Gather(DZ, s2, r2, rows, chunks)
    ga.start()
    loads[0].wait()
    for c in range(3):
        WQ[c] = W3[:, c, :]
    outs = [pltpu.make_async_copy(WQ, wq_o, ls.at[2])]
    outs[0].start()

    def project(n, carry):
        @pl.when(n == 1)
        def _():
            ga.side.wait_recv()

        @pl.when(n == 2)
        def _():
            for k in range(chunks):
                ga.relay(k)
            gz.start()

        @pl.when(n == 3)
        def _():
            for k in range(chunks):
                ga.fwd[k].wait_recv()

        here = block(order_of(n, (t, sib, yp, far)), rows)
        for c, (ref, cat) in enumerate(((QC, cat_q), (KC, cat_k), (VC, cat_k))):
            pr = mm(A[here, :], WQ[c])
            if c == 0:
                pr = pr * (1.0 / math.sqrt(HD))
            for h in range(heads):
                ref[h, here, :] = cat(pr[:, h * HD : (h + 1) * HD])
        return carry

    lax.fori_loop(0, 4, project, 0)
    more = [
        pltpu.make_async_copy(A, a_o, ls.at[3]),
        pltpu.make_async_copy(QC, qc_o, ls.at[4]),
        pltpu.make_async_copy(KC, kc_o, ls.at[5]),
        pltpu.make_async_copy(VC, vc_o, ls.at[6]),
    ]
    for c in more:
        c.start()
    outs += more
    loads[1].wait()
    blocks = slots // QB
    row = lax.broadcasted_iota(jnp.int32, (QB, QB), 0)
    col = lax.broadcasted_iota(jnp.int32, (QB, QB), 1)
    upper = t // 2
    rs = Scatter(PT, OWN, PRE, YIN, s3, r3, rows, chunks)

    def attend(n, carry):
        i = upper * n + (1 - upper) * (blocks - 1 - n)
        q_rows = pl.ds(pl.multiple_of(i * QB, QB), QB)
        TOP[...] = jnp.full(TOP.shape, -HUGE, f32)
        SUM[...] = jnp.zeros(SUM.shape, f32)
        OT[...] = jnp.zeros(OT.shape, f32)

        def keys(j, inner):
            k_rows = pl.ds(pl.multiple_of(j * QB, QB), QB)
            ok = (row <= col) | (j < i)
            for h in range(heads):
                s = jnp.where(ok, bdot(KC[h, k_rows, :], QC[h, q_rows, :], NT), -HUGE)
                old = TOP[h]
                new = jnp.maximum(old, jnp.max(s, 0, keepdims=True))
                shrink = jnp.exp(old - new)
                p = jnp.exp(s - new)
                TOP[h] = new
                SUM[h] = SUM[h] * shrink + jnp.sum(p, 0, keepdims=True)
                ph, pw = halves(p)
                values = VC[h, k_rows, 0 : 2 * HD]
                OT[h] = OT[h] * shrink + (bdot(values, ph, TN) + bdot(values, pw, TN))
            return inner

        lax.fori_loop(0, i + 1, keys, 0)
        parts = []
        for h in range(heads):
            parts.append((OT[h, :HD, :] + OT[h, HD:, :]) / SUM[h])
            LSE[h, :, q_rows] = TOP[h] + jnp.log(SUM[h])
        o = jnp.concatenate(parts, axis=0).T
        O[q_rows, :] = o
        PT[q_rows, :] = mm(o, WO[...])

        @pl.when(n == 2)
        def _():
            for k in range(chunks):
                rs.send_pre(k)

        @pl.when(n == 3)
        def _():
            for k in range(chunks):
                rs.send_across(k)
            gz.side.wait_recv()

        return carry

    lax.fori_loop(0, blocks, attend, 0)
    rs.send_side()
    for k in range(chunks):
        gz.relay(k)
    more = [pltpu.make_async_copy(O, o_o, ls.at[7]), pltpu.make_async_copy(LSE, lse_o, ls.at[8])]
    for c in more:
        c.start()
    outs += more
    for k in range(chunks):
        gz.fwd[k].wait_recv()
    more = [pltpu.make_async_copy(DZ, dz_o, ls.at[9])]
    more[0].start()
    outs += more
    rs.arrive()
    gain2, bias2 = row_of(g2), row_of(b2)

    def end_rows(r):
        here = pl.ds(r, RS)
        _, live = slot_facts(mine0 + r, passes)
        h1 = h1_o[here, :] + live * rs.total(r, RS)
        h1_o[here, :] = h1
        xhat, _ = norm_stats(h1)
        c_o[here, :] = xhat * gain2 + bias2

    over_rows(rows, end_rows)
    for c in outs:
        c.wait()
    ga.finish_sends()
    gz.finish_sends()
    rs.finish_sends()


def struct(*shape):
    return jax.ShapeDtypeStruct(shape, f32)


def vm(*shape):
    return pltpu.VMEM(shape, f32)


def vb(*shape):
    return pltpu.VMEM(shape, bf16)


def pairs(count, *numbers):
    return [pltpu.SemaphoreType.DMA((n,)) for n in numbers for _ in range(count)]


IN_VMEM = pl.BlockSpec(memory_space=pltpu.VMEM)
IN_SMEM = pl.BlockSpec(memory_space=pltpu.SMEM)
IN_HBM = pl.BlockSpec(memory_space=pl.ANY)
CHUNKS = 2


def params(number):
    return pltpu.CompilerParams(collective_id=number, has_side_effects=True, vmem_limit_bytes=63 << 20)


def forward_call(passes, x, table, g1, b1, g2, b2, go, w, wo, slots):
    rows, feats = x.shape
    local = w.shape[2]
    heads = local // HD
    cat = jax.ShapeDtypeStruct((heads, slots, 4 * HD), bf16)
    ng = 1 + 2 * CHUNKS
    return pl.pallas_call(
        functools.partial(forward_kernel, (rows, slots, feats, heads, CHUNKS)),
        out_shape=(
            struct(slots, feats), cat, cat, cat, struct(slots, local), struct(heads, 1, slots), struct(3, feats, local),
            struct(rows, feats), struct(rows, feats), struct(slots, feats),
        ),
        in_specs=[IN_SMEM] + [IN_VMEM] * 7 + [IN_HBM] * 2,
        out_specs=(IN_HBM,) * 7 + (IN_VMEM, IN_VMEM, IN_HBM),
        scratch_shapes=[
            vm(slots, feats), vm(slots, feats),
            vb(heads, slots, 4 * HD), vb(heads, slots, 4 * HD), vb(heads, slots, 4 * HD),
            vm(slots, local), vm(heads, 1, slots), vm(heads, 1, QB), vm(heads, 1, QB), vm(heads, 2 * HD, QB), vm(slots, feats),
            vm(rows, feats), vm(rows, feats), vm(rows, feats),
            vm(feats, 3, local), vm(3, feats, local), vm(local, feats),
        ] + pairs(2, ng, ng, ng) + pairs(1, 10),
        compiler_params=params(1),
        name="forward_part",
    )(passes, x, table, g1, b1, g2, b2, go, w, wo)


def gelu_both(u):
    k = math.sqrt(2.0 / math.pi)
    square = u * u
    th = jnp.tanh(k * (u * (1.0 + 0.044715 * square)))
    half = 0.5 * (1.0 + th)
    slope = half + (0.5 * k) * u * (1.0 - th * th) * (1.0 + (3.0 * 0.044715) * square)
    return u * half, slope


def middle_kernel(
    dims, h1, go, g2, c_h, dz_h, wu_h, wd_h,
    dh1_o, vec_o, zp_o, gd_o, gu_o,
    C, DZ, ACT, DU, PT, OWN, PRE, YIN, WU, WD, GD, GU,
    s1, r1, s2, r2, ls,
):
    rows, slots, feats, chunks = dims
    t, sib, yp, far = places()
    first = pltpu.make_async_copy(c_h, C.at[block(t, rows)], ls.at[0])
    loads = [
        pltpu.make_async_copy(wd_h, WD, ls.at[1]),
        pltpu.make_async_copy(dz_h, DZ, ls.at[2]),
        pltpu.make_async_copy(wu_h, WU, ls.at[3]),
    ]
    first.start()
    for c in loads:
        c.start()
    greet([{"tensor": sib}, {"tensor": yp}])
    first.wait()
    gc = Gather(C, s1, r1, rows, chunks)
    gc.start()
    for c in loads:
        c.wait()

    def open_block(i, carry):
        here = block(i, rows)
        DU[here, :] = mm(DZ[here, :], WD[...], NT)
        return carry

    lax.fori_loop(0, slots // rows, open_block, 0)

    def work(here):
        act, slope = gelu_both(mm(C[here, :], WU[...]))
        ACT[here, :] = act
        du = DU[here, :] * slope
        DU[here, :] = du
        PT[here, :] = mm(du, WU[...], NT)

    rs = Scatter(PT, OWN, PRE, YIN, s2, r2, rows, chunks)

    def step(n, carry):
        @pl.when(n == 2)
        def _():
            gc.side.wait_recv()

        for k in range(chunks):

            @pl.when(n == 4 + 2 * k)
            def _():
                gc.relay(k)
                gc.fwd[k].wait_recv()

        late = n // 4
        k = late * ((n % 4) // 2) + (1 - late) * (n % 2)
        owner = late * ((n % 2) * yp + (1 - n % 2) * far) + (1 - late) * ((n // 2) * sib + (1 - n // 2) * t)
        here = pl.ds(pl.multiple_of(owner * rows + k * (rows // chunks), 8), rows // chunks)
        act, slope = gelu_both(mm(C[here, :], WU[...]))
        ACT[here, :] = act
        du = DU[here, :] * slope
        DU[here, :] = du
        PT[here, :] = mm(du, WU[...], NT)

        @pl.when(n == 3)
        def _():
            rs.send_side()

        for k in range(chunks):

            @pl.when(n == 4 + 2 * k)
            def _():
                rs.send_pre(k)

            @pl.when(n == 5 + 2 * k)
            def _():
                rs.send_across(k)

        return carry

    lax.fori_loop(0, 4 + 2 * chunks, step, 0)

    def grads(n, carry):
        cols = pl.ds(pl.multiple_of(n * 256, 256), 256)
        GU[cols, :] = mm(C[:, cols], DU[...], TN)
        GD[cols, :] = mm(DZ[:, cols], ACT[...], TN)
        return carry

    lax.fori_loop(0, feats // 256, grads, 0)
    gu_copy = pltpu.make_async_copy(GU, gu_o, ls.at[4])
    gu_copy.start()
    gd_copy = pltpu.make_async_copy(GD, gd_o, ls.at[5])
    gd_copy.start()

    def down(i, carry):
        here = block(i, rows)
        DZ[here, :] = mm(ACT[here, :], WD[...])
        return carry

    lax.fori_loop(0, slots // rows, down, 0)
    zp_copy = pltpu.make_async_copy(DZ, zp_o, ls.at[6])
    zp_copy.start()
    vec_o[...] = jnp.zeros_like(vec_o)
    gain2 = row_of(g2)
    rs.arrive()

    def end_rows(r):
        here = pl.ds(r, RS)
        dc = rs.total(r, RS)
        xhat, scale = norm_stats(h1[here, :])
        add_eight(vec_o, 0, dc * xhat)
        add_eight(vec_o, 8, dc)
        e = dc * gain2
        inner = e - jnp.mean(e, -1, keepdims=True) - xhat * jnp.mean(e * xhat, -1, keepdims=True)
        dh1_o[here, :] = go[here, :] + inner * scale

    over_rows(rows, end_rows)
    for c in (gu_copy, gd_copy, zp_copy):
        c.wait()
    gc.finish_sends()
    rs.finish_sends()


def middle_call(h1, go, g2, c, dz, wu, wd):
    rows, feats = h1.shape
    slots = dz.shape[0]
    hidden = wu.shape[1]
    ng = 1 + 2 * CHUNKS
    return pl.pallas_call(
        functools.partial(middle_kernel, (rows, slots, feats, CHUNKS)),
        out_shape=(struct(rows, feats), struct(16, feats), struct(slots, feats), struct(feats, hidden), struct(feats, hidden)),
        in_specs=[IN_VMEM] * 3 + [IN_HBM] * 4,
        out_specs=(IN_VMEM, IN_VMEM, IN_HBM, IN_HBM, IN_HBM),
        scratch_shapes=[
            vm(slots, feats), vm(slots, feats), vm(slots, hidden), vm(slots, hidden), vm(slots, feats),
            vm(rows, feats), vm(rows, feats), vm(rows, feats),
            vm(feats, hidden), vm(hidden, feats), vm(feats, hidden), vm(feats, hidden),
        ] + pairs(2, ng, ng) + pairs(1, 7),
        compiler_params=params(2),
        name="middle_part",
    )(h1, go, g2, c, dz, wu, wd)


FF_ORDERS = ((0, 1, 2), (1, 2, 0), (0, 1, 2), (0, 1, 2))
FF_START = (1, 0, 2, 3)
Q_ORDERS = ((0, 1, 2), (1, 0, 2), (0, 1, 2))


class Halve:
    def __init__(self, source, keep, in_one, in_two, in_three, send, recv, base, order):
        d = lax.axis_index("dp")
        bits = (d % 2, (d // 2) % 2, d // 4)
        peers = ({"dp": d + 1 - 2 * bits[0]}, {"dp": d + 2 - 4 * bits[1]}, {"dp": (d + 4) % 8})
        a1, a2, a3 = order
        self.mid, self.last = bits[a2], bits[a3]
        self.spot = (lambda x, y: 2 * x + y) if a2 > a3 else (lambda x, y: 2 * y + x)
        self.keep, self.ins = keep, (in_one, in_two, in_three)

        def whole(v, x, y):
            return v * 2**a1 + x * 2**a2 + y * 2**a3

        pick = [(x, y) for x in range(2) for y in range(2)]
        self.own = [(whole(bits[a1], x, y), self.spot(x, y)) for x, y in pick]
        self.one = [
            rcopy(source.at[whole(1 - bits[a1], x, y)], in_one.at[self.spot(x, y)], send.at[base + n], recv.at[base + n], peers[a1])
            for n, (x, y) in enumerate(pick)
        ]
        self.two = [
            rcopy(keep.at[self.spot(1 - self.mid, y)], in_two.at[y], send.at[base + 4 + y], recv.at[base + 4 + y], peers[a2])
            for y in range(2)
        ]
        self.three = rcopy(keep.at[self.spot(self.mid, 1 - self.last)], in_three, send.at[base + 6], recv.at[base + 6], peers[a3])

    def start_one(self):
        for c in self.one:
            c.start()

    def take_one(self):
        for c in self.one:
            c.wait_recv()
        self.keep[...] = self.keep[...] + self.ins[0][...]
        for c in self.two:
            c.start()

    def take_two(self):
        for y in range(2):
            self.two[y].wait_recv()
            at = self.spot(self.mid, y)
            self.keep[at] = self.keep[at] + self.ins[1][y]
        self.three.start()

    def take_three(self):
        self.three.wait_recv()
        return self.keep[self.spot(self.mid, self.last)] + self.ins[2][...]

    def finish_sends(self):
        for c in self.one + self.two + [self.three]:
            c.wait_send()


def backward_kernel(dims, *refs):
    rows, slots, feats, heads, chunks, halving = dims
    refs = list(refs)

    def take(n):
        out = refs[:n]
        del refs[:n]
        return out

    passes, x, table, g1, h1, dh1, vec2 = take(7)
    qc_h, kc_h, vc_h, o_h, lse_h, a_h, zp_h, wq_h, wo_h = take(9)
    if halving:
        gd_h, gu_h = take(2)
    out_o, gi_o, vec_o, gt_o, gq_o = take(5)
    if halving:
        gd_o, gu_o = take(2)
    QC, KC, VC, DOC, LSE, DROW, DATT, DQ, DK, DV, DP = take(11)
    OWN, PRE, YIN, ZP, ZOWN, ZPRE, ZYIN, WQ, WO, ACC, VB, VIN = take(12)
    if halving:
        GT, GQ, KF, KT, KQ, F1, F2, F3, T1, T2, T3, Q1, Q2, Q3 = take(14)
    s1, r1, s2, r2, s3, r3, sv, rv, ls = take(9)
    if halving:
        sh, rh = take(2)
    O = DP.at[0]
    t, sib, yp, far = places()
    mine0 = t * rows
    loads = [
        pltpu.make_async_copy(src, dst, ls.at[n])
        for n, (src, dst) in enumerate(
            ((wo_h, WO), (o_h, DP.at[0]), (zp_h, ZP), (qc_h, QC), (kc_h, KC), (vc_h, VC), (lse_h, LSE), (wq_h, WQ))
        )
    ]
    if halving:
        d = lax.axis_index("dp")
        low = d % 2
        width = KF.shape[-1]
        pieces = [(ref, k) for ref in (gu_h, gd_h) for k in range(ref.shape[-1] // width)]
        hf = []
        for n, (ref, k) in enumerate(pieces):
            ref = ref.at[:, :, pl.ds(k * width, width)]
            hf.append(Halve(ref, KF.at[n], F1.at[n], F2.at[n], F3.at[n], sh, rh, 7 * n, FF_ORDERS[n]))
            loads += [
                pltpu.make_async_copy(ref.at[a], KF.at[n, b], ls.at[9 + 4 * n + m]) for m, (a, b) in enumerate(hf[n].own)
            ]
        early = loads[8:]
    for c in loads:
        c.start()

    def begin_rows(r):
        here = pl.ds(r, RS)
        _, live = slot_facts(mine0 + r, passes)
        DATT[pl.ds(pl.multiple_of(mine0 + r, RS), RS), :] = live * dh1[here, :]

    over_rows(rows, begin_rows)
    others = [{"tensor": sib}, {"tensor": yp}]
    if halving:
        others += [{"dp": d + 1 - 2 * low}, {"dp": d + 2 - 4 * ((d // 2) % 2)}, {"dp": (d + 4) % 8}]
    greet(others)
    gt = Gather(DATT, s1, r1, rows, chunks)
    gt.start()
    if halving:
        for n in FF_START:
            hf[n].start_one()
        base = 7 * len(pieces)
        ht = Halve(GT, KT, T1, T2, T3, sh, rh, base, (0, 1, 2))
        hq = [Halve(GQ.at[c], KQ.at[c], Q1.at[c], Q2.at[c], Q3.at[c], sh, rh, base + 7 + 7 * c, Q_ORDERS[c]) for c in range(3)]

        def ff_out(n):
            k = n % (len(pieces) // 2)
            if n < len(pieces) // 2:
                gu_o[:, k * width : (k + 1) * width] = hf[n].take_three()
            else:
                gd_o[k * width : (k + 1) * width, :] = hf[n].take_three().T
    rz = Scatter(ZP, ZOWN, ZPRE, ZYIN, s2, r2, rows, chunks)
    loads[2].wait()
    for k in range(chunks):
        rz.send_pre(k)
    rz.send_side()
    loads[0].wait()

    def mixed_grad(n, carry):
        @pl.when(n == 1)
        def _():
            gt.side.wait_recv()

        @pl.when(n == 2)
        def _():
            for k in range(chunks):
                gt.relay(k)
            for k in range(chunks):
                rz.send_across(k)
            if halving:
                for c in early:
                    c.wait()
                hf[0].take_one()
                hf[1].take_one()

        @pl.when(n == 3)
        def _():
            for k in range(chunks):
                gt.fwd[k].wait_recv()

        here = block(order_of(n, (t, sib, yp, far)), rows)
        do = mm(DATT[here, :], WO[...], NT)
        for h in range(heads):
            DOC[h, here, :] = cat_q(do[:, h * HD : (h + 1) * HD])
        return carry

    lax.fori_loop(0, 4, mixed_grad, 0)
    loads[1].wait()
    grad_out = mm(DATT[...], O[...], TN)
    for c in loads[3:8]:
        c.wait()
    if halving:
        GT[...] = grad_out.reshape(GT.shape)
        for a, b in ht.own:
            KT[b] = GT[a]
        ht.start_one()
    else:
        gt_o[...] = grad_out
    gt.finish_sends()
    blocks = slots // QB
    row = lax.broadcasted_iota(jnp.int32, (QB, QB), 0)
    col = lax.broadcasted_iota(jnp.int32, (QB, QB), 1)
    ones = jnp.ones((8, HD), f32)
    for i in reversed(range(blocks)):
        q_rows = pl.ds(i * QB, QB)
        size = (i + 1) * QB
        k_rows = pl.ds(0, size)
        for h in range(heads):
            do = fold(DOC[h, q_rows, 0 : 2 * HD].astype(f32))
            DROW[h] = mm(ones, do * O[q_rows, h * HD : (h + 1) * HD], NT)

        def one_head(h, carry):
            q, do = QC[h, q_rows, :], DOC[h, q_rows, :]
            s = bdot(KC[h, k_rows, :], q, NT)
            last = jnp.where(row <= col, s[size - QB :, :], -HUGE)
            s = last if i == 0 else jnp.concatenate([s[: size - QB, :], last], axis=0)
            p = jnp.exp(s - LSE[h, :, q_rows])
            ds = p * (bdot(VC[h, k_rows, :], do, NT) - DROW[h, 0:1, :])
            ph, pw = halves(p)
            dsh, dsw = halves(ds)
            do2, q2 = do[:, : 2 * HD], q[:, : 2 * HD]
            dv = bdot(ph, do2) + bdot(pw, do2)
            dk = bdot(dsh, q2) + bdot(dsw, q2)
            keys = KC[h, k_rows, 0 : 2 * HD]
            DQ[h, :, :] = bdot(dsh, keys, TN) + bdot(dsw, keys, TN)
            if i == blocks - 1:
                DV[h, :, :] = dv
                DK[h, :, :] = dk
            else:
                DV[h, k_rows, :] = DV[h, k_rows, :] + dv
                DK[h, k_rows, :] = DK[h, k_rows, :] + dk
            return carry

        lax.fori_loop(0, heads, one_head, 0)
        dq = jnp.concatenate([fold(DQ[h]) for h in range(heads)], axis=1)
        DP[0, q_rows, :] = dq * (1.0 / math.sqrt(HD))
        if halving and i == 4:
            hf[0].take_two()
            hf[1].take_two()
        if halving and i == 3:
            hf[2].take_one()
        if halving and i == 2:
            ff_out(0)
        if halving and i == 1:
            ff_out(1)
            hf[2].take_two()
        if halving and i == 0:
            hf[3].take_one()
    rd = Scatter(DATT, OWN, PRE, YIN, s3, r3, rows, chunks)

    def head_grads(n, carry):
        here = block(order_of(n, (far, yp, sib, t)), rows)
        total = mm(DP[0, here, :], WQ[0], NT)
        for c, ref in ((1, DK), (2, DV)):
            part = jnp.concatenate([fold(ref[h, here, :]) for h in range(heads)], axis=1)
            DP[c, here, :] = part
            total = total + mm(part, WQ[c], NT)
        DATT[here, :] = total

        @pl.when(n == 0)
        def _():
            for k in range(chunks):
                rd.send_pre(k)

        @pl.when(n == 1)
        def _():
            for k in range(chunks):
                rd.send_across(k)

        @pl.when(n == 2)
        def _():
            rd.send_side()

        return carry

    lax.fori_loop(0, 4, head_grads, 0)
    rz.arrive()

    def out_rows(r):
        here = pl.ds(r, RS)
        _, live = slot_facts(mine0 + r, passes)
        out_o[here, :] = h1[here, :] + live * rz.total(r, RS)

    over_rows(rows, out_rows)
    rz.finish_sends()
    a_copy = pltpu.make_async_copy(a_h, ZP, ls.at[8])
    a_copy.start()
    a_copy.wait()

    def weight_grads(c, carry):
        full = mm(ZP[...], DP[c], TN)
        if not halving:
            gq_o[c] = full
            return carry
        GQ[c] = full.reshape(GQ.shape[1:])
        for k in range(3):

            @pl.when(c == k)
            def _():
                for a, b in hq[k].own:
                    KQ[k, b] = GQ[k, a]
                hq[k].start_one()

        return carry

    lax.fori_loop(0, 3, weight_grads, 0)
    if halving:
        hf[3].take_two()
        ff_out(2)
        ht.take_one()
        hq[1].take_one()
        hq[0].take_one()
        ff_out(3)
        ht.take_two()
        hq[1].take_two()
        hq[0].take_two()
        hq[2].take_one()
        gt_o[...] = ht.take_three().T
    ACC[...] = jnp.zeros_like(ACC)
    gain1 = row_of(g1)
    rd.arrive()

    def end_rows(r):
        here = pl.ds(r, RS)
        which, _ = slot_facts(mine0 + r, passes)
        xhat, scale = norm_stats(embed(x, which, table, here))
        da = rd.total(r, RS)
        add_eight(ACC, 0, da * xhat)
        add_eight(ACC, 8, da)
        e = da * gain1
        inner = e - jnp.mean(e, -1, keepdims=True) - xhat * jnp.mean(e * xhat, -1, keepdims=True)
        gi = dh1[here, :] + inner * scale
        gi_o[here, :] = gi
        for p in range(PASSES_MAX):
            add_eight(ACC, 16 + 8 * p, jnp.where(which == p, gi, 0.0))

    over_rows(rows, end_rows)
    VB[0] = jnp.zeros_like(VB[0])
    for n in range(2):
        VB[0, pl.ds(n, 1), :] = jnp.sum(ACC[8 * n : 8 * n + 8, :], 0, keepdims=True)
        VB[0, pl.ds(2 + n, 1), :] = jnp.sum(vec2[8 * n : 8 * n + 8, :], 0, keepdims=True)
    for p in range(PASSES_MAX):
        VB[0, pl.ds(4 + p, 1), :] = jnp.sum(ACC[16 + 8 * p : 24 + 8 * p, :], 0, keepdims=True)
    rounds = []
    for n, other in enumerate(others):
        c = rcopy(VB.at[n], VIN.at[n], sv.at[n], rv.at[n], other)
        c.start()
        if halving and n == 0:
            hq[2].take_two()
        if halving and n == 1:
            gq_o[:, 0, :] = hq[0].take_three()
        if halving and n == 2:
            gq_o[:, 1, :] = hq[1].take_three()
        c.wait_recv()
        VB[n + 1] = VB[n] + VIN[n]
        rounds.append(c)
    if halving:
        share = feats // 8
        for k in range(8):

            @pl.when(d == k)
            def _():
                vec_o[...] = VB[len(others), :, k * share : (k + 1) * share]

        gq_o[:, 2, :] = hq[2].take_three()
        for h in hf + [ht] + hq:
            h.finish_sends()
    else:
        vec_o[...] = VB[len(others)]
    for c in rounds:
        c.wait_send()
    rd.finish_sends()


def backward_call(passes, x, table, g1, h1, dh1, vec2, qc, kc, vc, o, lse, a, zp, wq, wo, gd, gu, halving):
    rows, feats = x.shape
    slots, local = o.shape
    heads = local // HD
    hidden = gd.shape[1]
    ng = 1 + 2 * CHUNKS
    ends = 5 if halving else 2
    share = feats // 8
    cat = vb(heads, slots, 4 * HD)
    wide = vm(heads, slots, 2 * HD)
    outs = [struct(rows, feats), struct(rows, feats), struct(16, share if halving else feats)]
    args = [passes, x, table, g1, h1, dh1, vec2, qc, kc, vc, o, lse, a, zp, wq, wo]
    scratch = [
        cat, cat, cat, cat, vm(heads, 1, slots), vm(heads, 8, QB), vm(slots, feats), vm(heads, QB, 2 * HD), wide, wide, vm(3, slots, local),
        vm(rows, feats), vm(rows, feats), vm(rows, feats), vm(slots, feats), vm(rows, feats), vm(rows, feats), vm(rows, feats),
        vm(3, feats, local), vm(local, feats), vm(16 + 8 * PASSES_MAX, feats), vm(ends + 1, 16, feats), vm(ends, 16, feats),
    ]
    sems = pairs(2, ng, ng, ng, ends) + pairs(1, 25)
    if halving:
        outs += [struct(local, share), struct(share, 3, local), struct(hidden, share), struct(share, hidden)]
        args += [gd.reshape(8, share, hidden), gu.reshape(8, share, hidden)]
        scratch += [vm(8, share, local), vm(3, 8, share, local)]
        width = hidden // 2
        scratch += [vm(4, 4, share, width), vm(4, share, local), vm(3, 4, share, local)]
        scratch += [vm(4, 4, share, width), vm(4, 2, share, width), vm(4, share, width)]
        scratch += [vm(4, share, local), vm(2, share, local), vm(share, local)]
        scratch += [vm(3, 4, share, local), vm(3, 2, share, local), vm(3, share, local)]
        sems += pairs(2, 56)
    else:
        outs += [struct(feats, local), struct(3, feats, local)]
    return pl.pallas_call(
        functools.partial(backward_kernel, (rows, slots, feats, heads, CHUNKS, halving)),
        out_shape=tuple(outs),
        in_specs=[IN_SMEM] + [IN_VMEM] * 6 + [IN_HBM] * (len(args) - 7),
        out_specs=(IN_VMEM,) * len(outs),
        scratch_shapes=scratch + sems,
        compiler_params=params(3),
        name="backward_part",
    )(*args)


def per_device(
    block_input, passes, pass_map, pass_table, gain_one, bias_one, w_qkv, w_out, gain_two, bias_two, w_up, w_down, grad_output
):
    x, go = block_input[0], grad_output[0]
    rows, feats = x.shape
    slots = rows * lax.axis_size("tensor")
    ways = lax.axis_size("dp")
    halving = ways == 8
    a, qc, kc, vc, o, lse, wq, h1, c, dz = forward_call(
        passes, x, pass_table, gain_one, bias_one, gain_two, bias_two, go, w_qkv, w_out, slots
    )
    dh1, vec2, zp, gd, gu = middle_call(h1, go, gain_two, c, dz, w_up, w_down)
    got = backward_call(passes, x, pass_table, gain_one, h1, dh1, vec2, qc, kc, vc, o, lse, a, zp, wq, w_out, gd, gu, halving)
    out, gi, part, gt, gq = got[:5]
    if halving:
        gd, gu = got[5:]
    else:
        gq = jnp.swapaxes(gq, 0, 1)
        gt, gq, gu, gd = (lax.psum_scatter(v, "dp", scatter_dimension=0, tiled=True) for v in (gt, gq, gu, gd))
        part = lax.psum_scatter(part, "dp", scatter_dimension=1, tiled=True)
        gt, gd = gt.T, gd.T
    return (
        out[None], gi[None], part[4 : 4 + PASSES_MAX], part[0], part[1], gq, gt, part[2], part[3], gu, gd,
    )


def solution(mesh):
    placed = (
        P("dp", "tensor", None), P("dp"), P("dp", "tensor"), P(), P(), P(), P(None, None, "tensor"), P("tensor", None),
        P(), P(), P(None, "tensor"), P("tensor", None), P("dp", "tensor", None),
    )
    return jax.shard_map(
        per_device,
        mesh=mesh,
        in_specs=placed,
        out_specs=(
            P("dp", "tensor", None), P("dp", "tensor", None), P(None, "dp"), P("dp"), P("dp"), P("dp", None, "tensor"),
            P("tensor", "dp"), P("dp"), P("dp"), P("dp", "tensor"), P("tensor", "dp"),
        ),
        check_vma=False,
    )
```

```python
import math
import functools
import jax
import jax.numpy as jnp
from jax import lax
from jax.experimental import pallas as pl
from jax.experimental.pallas import tpu as pltpu
from jax.sharding import PartitionSpec as P

f32 = jnp.float32
bf16 = jnp.bfloat16
HD = 64
BASE = 256
PASSES_MAX = 5
EPSILON = 1e-05
HUGE = 1e30
QB = 256
HIGH = lax.Precision.HIGH
MESH = pl.DeviceIdType.MESH
NN = (((1,), (0,)), ((), ()))
NT = (((1,), (1,)), ((), ()))
TN = (((0,), (0,)), ((), ()))


def mm(left, right, dims=NN):
    return lax.dot_general(left, right, dims, precision=HIGH, preferred_element_type=f32)


def bdot(left, right, dims=NN):
    return lax.dot_general(left, right, dims, preferred_element_type=f32)


def halves(value):
    high = value.astype(bf16)
    return high, (value - high.astype(f32)).astype(bf16)


def rcopy(src, dst, send, recv, where):
    return pltpu.make_async_remote_copy(
        src_ref=src, dst_ref=dst, send_sem=send, recv_sem=recv, device_id=where, device_id_type=MESH
    )


def places():
    t = lax.axis_index("tensor")
    sib = t + 1 - 2 * (t % 2)
    yp = (t + 2) % 4
    far = (sib + 2) % 4
    return t, sib, yp, far


def greet(others):
    for other in others:
        pl.semaphore_signal(pltpu.get_barrier_semaphore(), inc=1, device_id=other, device_id_type=MESH)


def met(others):
    pl.semaphore_wait(pltpu.get_barrier_semaphore(), len(others))


def order_of(n, owners):
    out = owners[0]
    for k in range(1, len(owners)):
        here = (n + len(owners) - k) // len(owners) - (n + len(owners) - k - 1) // len(owners)
        out = out + here * (owners[k] - owners[0])
    return out


def block(owner, rows, chunk=0, chunks=1):
    size = rows // chunks
    return pl.ds(pl.multiple_of(owner * rows + chunk * size, 8), size)


class Gather:
    def __init__(self, buf, send, recv, rows, chunks, source=None):
        t, sib, yp, far = places()
        self.own, self.yp, self.sib, self.far, self.rows, self.chunks = t, yp, sib, far, rows, chunks
        self.across, self.fwd = [], []
        mine = buf.at[block(t, rows)]
        self.side = rcopy(mine if source is None else source, mine, send.at[0], recv.at[0], {"tensor": sib})
        for k in range(chunks):
            part = buf.at[block(t, rows, k, chunks)]
            first = part if source is None else source.at[pl.ds(k * (rows // chunks), rows // chunks)]
            self.across.append(rcopy(first, part, send.at[1 + k], recv.at[1 + k], {"tensor": yp}))
            part = buf.at[block(yp, rows, k, chunks)]
            j = 1 + chunks + k
            self.fwd.append(rcopy(part, part, send.at[j], recv.at[j], {"tensor": sib}))

    def start(self):
        for c in self.across:
            c.start()
        self.side.start()

    def relay(self, k):
        self.across[k].wait_recv()
        self.fwd[k].start()

    def finish_sends(self):
        self.side.wait_send()
        for c in self.across + self.fwd:
            c.wait_send()


class Scatter:
    def __init__(self, part, own_in, pre_in, y_in, send, recv, rows, chunks):
        t, sib, yp, far = places()
        self.part, self.own_in, self.pre_in, self.y_in = part, own_in, pre_in, y_in
        self.rows, self.chunks, self.size = rows, chunks, rows // chunks
        self.t, self.sib, self.yp, self.far = t, sib, yp, far
        self.side = rcopy(part.at[block(sib, rows)], own_in, send.at[0], recv.at[0], {"tensor": sib})
        self.pre, self.across = [], []
        for k in range(chunks):
            here = pl.ds(k * self.size, self.size)
            self.pre.append(
                rcopy(part.at[block(far, rows, k, chunks)], pre_in.at[here], send.at[1 + k], recv.at[1 + k], {"tensor": sib})
            )
            j = 1 + chunks + k
            self.across.append(rcopy(pre_in.at[here], y_in.at[here], send.at[j], recv.at[j], {"tensor": yp}))

    def send_pre(self, k):
        self.pre[k].start()

    def send_across(self, k):
        self.pre[k].wait_recv()
        here = pl.ds(k * self.size, self.size)
        self.pre_in[here, :] = self.part[block(self.yp, self.rows, k, self.chunks), :] + self.pre_in[here, :]
        self.across[k].start()

    def send_side(self):
        self.side.start()

    def arrive(self):
        self.side.wait_recv()
        for c in self.across:
            c.wait_recv()

    def total(self, start, size):
        here = pl.ds(start, size)
        mine = pl.ds(pl.multiple_of(self.t * self.rows + start, 8), size)
        return self.part[mine, :] + self.own_in[here, :] + self.y_in[here, :]

    def finish_sends(self):
        self.side.wait_send()
        for c in self.pre + self.across:
            c.wait_send()


def slot_facts(start, passes_ref):
    count = passes_ref[0]
    slot = start + lax.broadcasted_iota(jnp.int32, (RS, 1), 0)
    which = jnp.zeros_like(slot)
    for r in range(1, PASSES_MAX + 1):
        which = jnp.where(count == r, slot % r, which)
    return which, jnp.where(slot < count * BASE, 1.0, 0.0)


def embed(x_ref, which, table_ref, here):
    rows = x_ref[here, :]
    added = jnp.zeros_like(rows)
    for p in range(PASSES_MAX):
        added = jnp.where(which == p, table_ref[pl.ds(p, 1), :], added)
    return rows + added


def norm_stats(values):
    center = values - jnp.mean(values, -1, keepdims=True)
    spread = jnp.mean(center * center, -1, keepdims=True)
    scale = lax.rsqrt(spread + EPSILON)
    return center * scale, scale


RS = 32


def over_rows(rows, body, size=RS):
    def step(i, carry):
        body(pl.multiple_of(i * size, size))
        return carry

    lax.fori_loop(0, rows // size, step, 0)


def cat_q(v):
    high = v.astype(bf16).astype(f32)
    low = v - high
    return jnp.concatenate([high, low, low, high], axis=1).astype(bf16)


def cat_k(v):
    high = v.astype(bf16).astype(f32)
    low = v - high
    return jnp.concatenate([high, low, high, low], axis=1).astype(bf16)


def fold(both):
    return both[:, :HD] + both[:, HD:]


def causal(s, size):
    row = lax.broadcasted_iota(jnp.int32, (QB, QB), 0)
    col = lax.broadcasted_iota(jnp.int32, (QB, QB), 1)
    last = jnp.where(col <= row, s[:, size - QB :], -HUGE)
    return last if size == QB else jnp.concatenate([s[:, : size - QB], last], axis=1)


def add_eight(ref, row, value):
    total = value[0:8, :]
    for k in range(1, value.shape[0] // 8):
        total = total + value[8 * k : 8 * k + 8, :]
    ref[pl.ds(row, 8), :] = ref[pl.ds(row, 8), :] + total


def row_of(ref):
    return ref[...].reshape(1, ref.shape[0])


def forward_kernel(
    dims, passes, x, table, g1, b1, g2, b2, go, wq_h, wo_h,
    a_o, qc_o, kc_o, vc_o, o_o, lse_o, h1_o, c_o, dz_o,
    A, DZ, QC, KC, VC, O, LSE, TOP, SUM, OT, PT, OWN, PRE, YIN, WQ, WO,
    s1, r1, s2, r2, s3, r3, ls,
):
    rows, slots, feats, heads, chunks = dims
    t, sib, yp, far = places()
    mine0 = t * rows
    loads = [pltpu.make_async_copy(wq_h, WQ, ls.at[0]), pltpu.make_async_copy(wo_h, WO, ls.at[1])]
    for c in loads:
        c.start()
    gain, bias = row_of(g1), row_of(b1)

    others = [{"tensor": sib}, {"tensor": yp}]
    greet(others)
    ga = Gather(A, s1, r1, rows, chunks)
    gz = Gather(DZ, s2, r2, rows, chunks)

    def begin_rows(r):
        here = pl.ds(r, RS)
        which, _ = slot_facts(mine0 + r, passes)
        h0 = embed(x, which, table, here)
        h1_o[here, :] = h0
        xhat, _ = norm_stats(h0)
        A[pl.ds(pl.multiple_of(mine0 + r, RS), RS), :] = xhat * gain + bias

    over_rows(rows // 2, begin_rows)
    met(others)
    ga.across[0].start()
    over_rows(rows // 2, lambda r: begin_rows(r + rows // 2))
    ga.across[1].start()
    ga.side.start()

    def mask_rows(r):
        here = pl.ds(r, RS)
        _, live = slot_facts(mine0 + r, passes)
        DZ[pl.ds(pl.multiple_of(mine0 + r, RS), RS), :] = live * go[here, :]

    over_rows(rows, mask_rows)
    loads[0].wait()
    outs = []

    def project(n, carry):
        @pl.when(n == 1)
        def _():
            ga.side.wait_recv()

        @pl.when(n == 2)
        def _():
            for k in range(chunks):
                ga.relay(k)
            gz.start()

        @pl.when(n == 3)
        def _():
            for k in range(chunks):
                ga.fwd[k].wait_recv()

        here = block(order_of(n, (t, sib, yp, far)), rows)
        for c, (ref, cat) in enumerate(((QC, cat_q), (KC, cat_k), (VC, cat_k))):
            pr = mm(A[here, :], WQ[c], NT)
            if c == 0:
                pr = pr * (1.0 / math.sqrt(HD))
            for h in range(heads):
                ref[h, here, :] = cat(pr[:, h * HD : (h + 1) * HD])
        return carry

    lax.fori_loop(0, 4, project, 0)
    more = [
        pltpu.make_async_copy(A, a_o, ls.at[3]),
        pltpu.make_async_copy(QC, qc_o, ls.at[4]),
        pltpu.make_async_copy(KC, kc_o, ls.at[5]),
        pltpu.make_async_copy(VC, vc_o, ls.at[6]),
    ]
    for c in more:
        c.start()
    outs += more
    loads[1].wait()
    blocks = slots // QB
    row = lax.broadcasted_iota(jnp.int32, (QB, QB), 0)
    col = lax.broadcasted_iota(jnp.int32, (QB, QB), 1)
    upper = t // 2
    rs = Scatter(PT, OWN, PRE, YIN, s3, r3, rows, chunks)

    def attend(n, carry):
        i = upper * n + (1 - upper) * (blocks - 1 - n)
        q_rows = pl.ds(pl.multiple_of(i * QB, QB), QB)
        TOP[...] = jnp.full(TOP.shape, -HUGE, f32)
        SUM[...] = jnp.zeros(SUM.shape, f32)
        OT[...] = jnp.zeros(OT.shape, f32)

        def keys(j, inner):
            k_rows = pl.ds(pl.multiple_of(j * QB, QB), QB)
            ok = (row <= col) | (j < i)
            for h in range(heads):
                s = jnp.where(ok, bdot(KC[h, k_rows, :], QC[h, q_rows, :], NT), -HUGE)
                old = TOP[h]
                new = jnp.maximum(old, jnp.max(s, 0, keepdims=True))
                shrink = jnp.exp(old - new)
                p = jnp.exp(s - new)
                TOP[h] = new
                SUM[h] = SUM[h] * shrink + jnp.sum(p, 0, keepdims=True)
                ph, pw = halves(p)
                values = VC[h, k_rows, 0 : 2 * HD]
                OT[h] = OT[h] * shrink + (bdot(values, ph, TN) + bdot(values, pw, TN))
            return inner

        lax.fori_loop(0, i + 1, keys, 0)
        parts = []
        for h in range(heads):
            parts.append((OT[h, :HD, :] + OT[h, HD:, :]) / SUM[h])
            LSE[h, :, q_rows] = TOP[h] + jnp.log(SUM[h])
        o = jnp.concatenate(parts, axis=0).T
        O[q_rows, :] = o
        PT[q_rows, :] = mm(o, WO[...])

        @pl.when(n == 2)
        def _():
            for k in range(chunks):
                rs.send_pre(k)

        @pl.when(n == 3)
        def _():
            for k in range(chunks):
                rs.send_across(k)
            gz.side.wait_recv()

        return carry

    lax.fori_loop(0, blocks, attend, 0)
    rs.send_side()
    for k in range(chunks):
        gz.relay(k)
    more = [pltpu.make_async_copy(O, o_o, ls.at[7]), pltpu.make_async_copy(LSE, lse_o, ls.at[8])]
    for c in more:
        c.start()
    outs += more
    for k in range(chunks):
        gz.fwd[k].wait_recv()
    more = [pltpu.make_async_copy(DZ, dz_o, ls.at[9])]
    more[0].start()
    outs += more
    rs.arrive()
    gain2, bias2 = row_of(g2), row_of(b2)

    def end_rows(r):
        here = pl.ds(r, RS)
        _, live = slot_facts(mine0 + r, passes)
        h1 = h1_o[here, :] + live * rs.total(r, RS)
        h1_o[here, :] = h1
        xhat, _ = norm_stats(h1)
        c_o[here, :] = xhat * gain2 + bias2

    over_rows(rows, end_rows)
    for c in outs:
        c.wait()
    ga.finish_sends()
    gz.finish_sends()
    rs.finish_sends()


def struct(*shape):
    return jax.ShapeDtypeStruct(shape, f32)


def vm(*shape):
    return pltpu.VMEM(shape, f32)


def vb(*shape):
    return pltpu.VMEM(shape, bf16)


def pairs(count, *numbers):
    return [pltpu.SemaphoreType.DMA((n,)) for n in numbers for _ in range(count)]


IN_VMEM = pl.BlockSpec(memory_space=pltpu.VMEM)
IN_SMEM = pl.BlockSpec(memory_space=pltpu.SMEM)
IN_HBM = pl.BlockSpec(memory_space=pl.ANY)
CHUNKS = 2


def params(number):
    return pltpu.CompilerParams(collective_id=number, has_side_effects=True, vmem_limit_bytes=63 << 20)


def forward_call(passes, x, table, g1, b1, g2, b2, go, wq, wo, slots):
    rows, feats = x.shape
    local = wq.shape[1]
    heads = local // HD
    cat = jax.ShapeDtypeStruct((heads, slots, 4 * HD), bf16)
    ng = 1 + 2 * CHUNKS
    return pl.pallas_call(
        functools.partial(forward_kernel, (rows, slots, feats, heads, CHUNKS)),
        out_shape=(
            struct(slots, feats), cat, cat, cat, struct(slots, local), struct(heads, 1, slots),
            struct(rows, feats), struct(rows, feats), struct(slots, feats),
        ),
        in_specs=[IN_SMEM] + [IN_VMEM] * 7 + [IN_HBM] * 2,
        out_specs=(IN_HBM,) * 6 + (IN_VMEM, IN_VMEM, IN_HBM),
        scratch_shapes=[
            vm(slots, feats), vm(slots, feats),
            vb(heads, slots, 4 * HD), vb(heads, slots, 4 * HD), vb(heads, slots, 4 * HD),
            vm(slots, local), vm(heads, 1, slots), vm(heads, 1, QB), vm(heads, 1, QB), vm(heads, 2 * HD, QB), vm(slots, feats),
            vm(rows, feats), vm(rows, feats), vm(rows, feats),
            vm(3, local, feats), vm(local, feats),
        ] + pairs(2, ng, ng, ng) + pairs(1, 10),
        compiler_params=params(1),
        name="forward_part",
    )(passes, x, table, g1, b1, g2, b2, go, wq, wo)


def gelu_both(u):
    k = math.sqrt(2.0 / math.pi)
    square = u * u
    th = jnp.tanh(k * (u * (1.0 + 0.044715 * square)))
    half = 0.5 * (1.0 + th)
    slope = half + (0.5 * k) * u * (1.0 - th * th) * (1.0 + (3.0 * 0.044715) * square)
    return u * half, slope


def middle_kernel(
    dims, h1, go, g2, c_h, dz_h, wu_h, wd_h,
    dh1_o, vec_o, zp_o, gd_o, gu_o,
    C, DZ, ACT, DU, PT, OWN, PRE, YIN, WU, WD, GD, GU,
    s1, r1, s2, r2, ls,
):
    rows, slots, feats, chunks = dims
    t, sib, yp, far = places()
    first = pltpu.make_async_copy(c_h, C.at[block(t, rows)], ls.at[0])
    loads = [
        pltpu.make_async_copy(wd_h, WD, ls.at[1]),
        pltpu.make_async_copy(dz_h, DZ, ls.at[2]),
        pltpu.make_async_copy(wu_h, WU, ls.at[3]),
    ]
    first.start()
    for c in loads:
        c.start()
    others = [{"tensor": sib}, {"tensor": yp}]
    greet(others)
    gc = Gather(C, s1, r1, rows, chunks, c_h)
    met(others)
    gc.start()
    first.wait()
    for c in loads:
        c.wait()

    def open_block(i, carry):
        here = block(i, rows)
        DU[here, :] = mm(DZ[here, :], WD[...], NT)
        return carry

    lax.fori_loop(0, slots // rows, open_block, 0)

    def work(here):
        act, slope = gelu_both(mm(C[here, :], WU[...]))
        ACT[here, :] = act
        du = DU[here, :] * slope
        DU[here, :] = du
        PT[here, :] = mm(du, WU[...], NT)

    rs = Scatter(PT, OWN, PRE, YIN, s2, r2, rows, chunks)

    def step(n, carry):
        @pl.when(n == 2)
        def _():
            gc.side.wait_recv()

        for k in range(chunks):

            @pl.when(n == 4 + 2 * k)
            def _():
                gc.relay(k)
                gc.fwd[k].wait_recv()

        late = n // 4
        k = late * ((n % 4) // 2) + (1 - late) * (n % 2)
        owner = late * ((n % 2) * yp + (1 - n % 2) * far) + (1 - late) * ((n // 2) * sib + (1 - n // 2) * t)
        here = pl.ds(pl.multiple_of(owner * rows + k * (rows // chunks), 8), rows // chunks)
        act, slope = gelu_both(mm(C[here, :], WU[...]))
        ACT[here, :] = act
        du = DU[here, :] * slope
        DU[here, :] = du
        PT[here, :] = mm(du, WU[...], NT)

        @pl.when(n == 3)
        def _():
            rs.send_side()

        for k in range(chunks):

            @pl.when(n == 4 + 2 * k)
            def _():
                rs.send_pre(k)

            @pl.when(n == 5 + 2 * k)
            def _():
                rs.send_across(k)

        return carry

    lax.fori_loop(0, 4 + 2 * chunks, step, 0)

    def grads(n, carry):
        cols = pl.ds(pl.multiple_of(n * 256, 256), 256)
        GU[cols, :] = mm(C[:, cols], DU[...], TN)
        GD[cols, :] = mm(DZ[:, cols], ACT[...], TN)
        return carry

    lax.fori_loop(0, feats // 256, grads, 0)
    gu_copy = pltpu.make_async_copy(GU, gu_o, ls.at[4])
    gu_copy.start()
    gd_copy = pltpu.make_async_copy(GD, gd_o, ls.at[5])
    gd_copy.start()

    def down(i, carry):
        here = block(i, rows)
        DZ[here, :] = mm(ACT[here, :], WD[...])
        return carry

    lax.fori_loop(0, slots // rows, down, 0)
    zp_copy = pltpu.make_async_copy(DZ, zp_o, ls.at[6])
    zp_copy.start()
    vec_o[...] = jnp.zeros_like(vec_o)
    gain2 = row_of(g2)
    rs.arrive()

    def end_rows(r):
        here = pl.ds(r, RS)
        dc = rs.total(r, RS)
        xhat, scale = norm_stats(h1[here, :])
        add_eight(vec_o, 0, dc * xhat)
        add_eight(vec_o, 8, dc)
        e = dc * gain2
        inner = e - jnp.mean(e, -1, keepdims=True) - xhat * jnp.mean(e * xhat, -1, keepdims=True)
        dh1_o[here, :] = go[here, :] + inner * scale

    over_rows(rows, end_rows)
    for c in (gu_copy, gd_copy, zp_copy):
        c.wait()
    gc.finish_sends()
    rs.finish_sends()


def middle_call(h1, go, g2, c, dz, wu, wd):
    rows, feats = h1.shape
    slots = dz.shape[0]
    hidden = wu.shape[1]
    ng = 1 + 2 * CHUNKS
    return pl.pallas_call(
        functools.partial(middle_kernel, (rows, slots, feats, CHUNKS)),
        out_shape=(struct(rows, feats), struct(16, feats), struct(slots, feats), struct(feats, hidden), struct(feats, hidden)),
        in_specs=[IN_VMEM] * 3 + [IN_HBM] * 4,
        out_specs=(IN_VMEM, IN_VMEM, IN_HBM, IN_HBM, IN_HBM),
        scratch_shapes=[
            vm(slots, feats), vm(slots, feats), vm(slots, hidden), vm(slots, hidden), vm(slots, feats),
            vm(rows, feats), vm(rows, feats), vm(rows, feats),
            vm(feats, hidden), vm(hidden, feats), vm(feats, hidden), vm(feats, hidden),
        ] + pairs(2, ng, ng) + pairs(1, 7),
        compiler_params=params(2),
        name="middle_part",
    )(h1, go, g2, c, dz, wu, wd)


FF_ORDERS = ((0, 1, 2), (1, 2, 0), (0, 1, 2), (0, 1, 2))
FF_START = (1, 0, 2, 3)
Q_ORDERS = ((0, 1, 2), (1, 0, 2), (0, 1, 2))


class Halve:
    def __init__(self, source, keep, in_one, in_two, in_three, send, recv, base, order):
        d = lax.axis_index("dp")
        bits = (d % 2, (d // 2) % 2, d // 4)
        peers = ({"dp": d + 1 - 2 * bits[0]}, {"dp": d + 2 - 4 * bits[1]}, {"dp": (d + 4) % 8})
        a1, a2, a3 = order
        self.mid, self.last = bits[a2], bits[a3]
        self.spot = (lambda x, y: 2 * x + y) if a2 > a3 else (lambda x, y: 2 * y + x)
        self.keep, self.ins = keep, (in_one, in_two, in_three)

        def whole(v, x, y):
            return v * 2**a1 + x * 2**a2 + y * 2**a3

        pick = [(x, y) for x in range(2) for y in range(2)]
        self.own = [(whole(bits[a1], x, y), self.spot(x, y)) for x, y in pick]
        self.one = [
            rcopy(source.at[whole(1 - bits[a1], x, y)], in_one.at[self.spot(x, y)], send.at[base + n], recv.at[base + n], peers[a1])
            for n, (x, y) in enumerate(pick)
        ]
        self.two = [
            rcopy(keep.at[self.spot(1 - self.mid, y)], in_two.at[y], send.at[base + 4 + y], recv.at[base + 4 + y], peers[a2])
            for y in range(2)
        ]
        self.three = rcopy(keep.at[self.spot(self.mid, 1 - self.last)], in_three, send.at[base + 6], recv.at[base + 6], peers[a3])

    def start_one(self):
        for c in self.one:
            c.start()

    def take_one(self):
        for c in self.one:
            c.wait_recv()
        self.keep[...] = self.keep[...] + self.ins[0][...]
        for c in self.two:
            c.start()

    def take_two(self):
        for y in range(2):
            self.two[y].wait_recv()
            at = self.spot(self.mid, y)
            self.keep[at] = self.keep[at] + self.ins[1][y]
        self.three.start()

    def take_three(self):
        self.three.wait_recv()
        return self.keep[self.spot(self.mid, self.last)] + self.ins[2][...]

    def finish_sends(self):
        for c in self.one + self.two + [self.three]:
            c.wait_send()


def backward_kernel(dims, *refs):
    rows, slots, feats, heads, chunks, halving = dims
    refs = list(refs)

    def take(n):
        out = refs[:n]
        del refs[:n]
        return out

    passes, x, table, g1, h1, dh1, vec2 = take(7)
    qc_h, kc_h, vc_h, o_h, lse_h, a_h, zp_h, wq_h, wo_h = take(9)
    if halving:
        gd_h, gu_h = take(2)
    out_o, gi_o, vec_o, gt_o, gq_o = take(5)
    if halving:
        gd_o, gu_o = take(2)
    QC, KC, VC, DOC, LSE, DROW, DATT, DQ, DK, DV, DP = take(11)
    OWN, PRE, YIN, ZP, ZOWN, ZPRE, ZYIN, WQ, WO, ACC, VB, VIN = take(12)
    if halving:
        GT, GQ, KF, KT, KQ, F1, F2, F3, T1, T2, T3, Q1, Q2, Q3 = take(14)
    s1, r1, s2, r2, s3, r3, sv, rv, ls = take(9)
    if halving:
        sh, rh = take(2)
    O = DP.at[0]
    t, sib, yp, far = places()
    mine0 = t * rows
    loads = [
        pltpu.make_async_copy(src, dst, ls.at[n])
        for n, (src, dst) in enumerate(
            ((wo_h, WO), (o_h, DP.at[0]), (zp_h, ZP), (qc_h, QC), (kc_h, KC), (vc_h, VC), (lse_h, LSE), (wq_h, WQ))
        )
    ]
    if halving:
        d = lax.axis_index("dp")
        low = d % 2
        width = KF.shape[-1]
        pieces = [(ref, k) for ref in (gu_h, gd_h) for k in range(ref.shape[-1] // width)]
        hf = []
        for n, (ref, k) in enumerate(pieces):
            ref = ref.at[:, :, pl.ds(k * width, width)]
            hf.append(Halve(ref, KF.at[n], F1.at[n], F2.at[n], F3.at[n], sh, rh, 7 * n, FF_ORDERS[n]))
            loads += [
                pltpu.make_async_copy(ref.at[a], KF.at[n, b], ls.at[9 + 4 * n + m]) for m, (a, b) in enumerate(hf[n].own)
            ]
        early = loads[8:]
    for c in loads:
        c.start()

    others = [{"tensor": sib}, {"tensor": yp}]
    if halving:
        others += [{"dp": d + 1 - 2 * low}, {"dp": d + 2 - 4 * ((d // 2) % 2)}, {"dp": (d + 4) % 8}]
    greet(others)

    def begin_rows(r):
        here = pl.ds(r, RS)
        _, live = slot_facts(mine0 + r, passes)
        DATT[pl.ds(pl.multiple_of(mine0 + r, RS), RS), :] = live * dh1[here, :]

    over_rows(rows, begin_rows)
    met(others)
    gt = Gather(DATT, s1, r1, rows, chunks)
    gt.start()
    if halving:
        for n in FF_START:
            hf[n].start_one()
        base = 7 * len(pieces)
        ht = Halve(GT, KT, T1, T2, T3, sh, rh, base, (0, 1, 2))
        hq = [Halve(GQ.at[c], KQ.at[c], Q1.at[c], Q2.at[c], Q3.at[c], sh, rh, base + 7 + 7 * c, Q_ORDERS[c]) for c in range(3)]

        def ff_out(n):
            k = n % (len(pieces) // 2)
            if n < len(pieces) // 2:
                gu_o[:, k * width : (k + 1) * width] = hf[n].take_three()
            else:
                gd_o[:, k * width : (k + 1) * width] = hf[n].take_three()
    rz = Scatter(ZP, ZOWN, ZPRE, ZYIN, s2, r2, rows, chunks)
    loads[2].wait()
    for k in range(chunks):
        rz.send_pre(k)
    rz.send_side()
    loads[0].wait()

    def mixed_grad(n, carry):
        @pl.when(n == 1)
        def _():
            gt.side.wait_recv()

        @pl.when(n == 2)
        def _():
            for k in range(chunks):
                gt.relay(k)
            for k in range(chunks):
                rz.send_across(k)
            if halving:
                for c in early:
                    c.wait()
                hf[0].take_one()
                hf[1].take_one()

        @pl.when(n == 3)
        def _():
            for k in range(chunks):
                gt.fwd[k].wait_recv()

        here = block(order_of(n, (t, sib, yp, far)), rows)
        do = mm(DATT[here, :], WO[...], NT)
        for h in range(heads):
            DOC[h, here, :] = cat_q(do[:, h * HD : (h + 1) * HD])
        return carry

    lax.fori_loop(0, 4, mixed_grad, 0)
    loads[1].wait()
    grad_out = mm(DATT[...], O[...], TN)
    for c in loads[3:8]:
        c.wait()
    if halving:
        GT[...] = grad_out.reshape(GT.shape)
        for a, b in ht.own:
            KT[b] = GT[a]
        ht.start_one()
    else:
        gt_o[...] = grad_out
    gt.finish_sends()
    blocks = slots // QB
    row = lax.broadcasted_iota(jnp.int32, (QB, QB), 0)
    col = lax.broadcasted_iota(jnp.int32, (QB, QB), 1)
    ones = jnp.ones((8, HD), f32)
    for i in reversed(range(blocks)):
        q_rows = pl.ds(i * QB, QB)
        size = (i + 1) * QB
        k_rows = pl.ds(0, size)
        for h in range(heads):
            do = fold(DOC[h, q_rows, 0 : 2 * HD].astype(f32))
            DROW[h] = mm(ones, do * O[q_rows, h * HD : (h + 1) * HD], NT)

        def one_head(h, carry):
            q, do = QC[h, q_rows, :], DOC[h, q_rows, :]
            s = bdot(KC[h, k_rows, :], q, NT)
            last = jnp.where(row <= col, s[size - QB :, :], -HUGE)
            s = last if i == 0 else jnp.concatenate([s[: size - QB, :], last], axis=0)
            p = jnp.exp(s - LSE[h, :, q_rows])
            ds = p * (bdot(VC[h, k_rows, :], do, NT) - DROW[h, 0:1, :])
            ph, pw = halves(p)
            dsh, dsw = halves(ds)
            do2, q2 = do[:, : 2 * HD], q[:, : 2 * HD]
            dv = bdot(ph, do2) + bdot(pw, do2)
            dk = bdot(dsh, q2) + bdot(dsw, q2)
            keys = KC[h, k_rows, 0 : 2 * HD]
            DQ[h, :, :] = bdot(dsh, keys, TN) + bdot(dsw, keys, TN)
            if i == blocks - 1:
                DV[h, :, :] = dv
                DK[h, :, :] = dk
            else:
                DV[h, k_rows, :] = DV[h, k_rows, :] + dv
                DK[h, k_rows, :] = DK[h, k_rows, :] + dk
            return carry

        lax.fori_loop(0, heads, one_head, 0)
        dq = jnp.concatenate([fold(DQ[h]) for h in range(heads)], axis=1)
        DP[0, q_rows, :] = dq * (1.0 / math.sqrt(HD))
        if halving and i == 4:
            hf[0].take_two()
            hf[1].take_two()
        if halving and i == 3:
            hf[2].take_one()
        if halving and i == 2:
            ff_out(0)
        if halving and i == 1:
            ff_out(1)
            hf[2].take_two()
        if halving and i == 0:
            hf[3].take_one()
    rd = Scatter(DATT, OWN, PRE, YIN, s3, r3, rows, chunks)

    rz.arrive()

    def out_rows(r):
        here = pl.ds(r, RS)
        _, live = slot_facts(mine0 + r, passes)
        out_o[here, :] = h1[here, :] + live * rz.total(r, RS)

    over_rows(rows, out_rows)
    rz.finish_sends()
    a_copy = pltpu.make_async_copy(a_h, ZP, ls.at[8])
    a_copy.start()

    def gather_heads(n, carry):
        here = block(n, rows)
        for c, ref in ((1, DK), (2, DV)):
            DP[c, here, :] = jnp.concatenate([fold(ref[h, here, :]) for h in range(heads)], axis=1)
        return carry

    lax.fori_loop(0, 4, gather_heads, 0)

    def head_grads(n, carry):
        here = block(order_of(n, (far, yp, sib, t)), rows)
        DATT[here, :] = mm(DP[0, here, :], WQ[0]) + mm(DP[1, here, :], WQ[1]) + mm(DP[2, here, :], WQ[2])

        @pl.when(n == 0)
        def _():
            for k in range(chunks):
                rd.send_pre(k)

        @pl.when(n == 1)
        def _():
            for k in range(chunks):
                rd.send_across(k)

        @pl.when(n == 2)
        def _():
            rd.send_side()

        return carry

    lax.fori_loop(0, 2, head_grads, 0)
    a_copy.wait()

    def weight_grads(c, carry):
        full = mm(ZP[...], DP[c], TN)
        if not halving:
            gq_o[c] = full
            return carry
        GQ[c] = full.reshape(GQ.shape[1:])
        for k in range(3):

            @pl.when(c == k)
            def _():
                for a, b in hq[k].own:
                    KQ[k, b] = GQ[k, a]
                hq[k].start_one()

        return carry

    lax.fori_loop(0, 3, weight_grads, 0)
    lax.fori_loop(2, 4, head_grads, 0)
    if halving:
        hf[3].take_two()
        ff_out(2)
        ht.take_one()
        hq[1].take_one()
        hq[0].take_one()
        ff_out(3)
        ht.take_two()
        hq[1].take_two()
        hq[0].take_two()
        hq[2].take_one()
        gt_o[...] = ht.take_three().T
    ACC[...] = jnp.zeros_like(ACC)
    gain1 = row_of(g1)
    rd.arrive()

    def end_rows(r):
        here = pl.ds(r, RS)
        which, _ = slot_facts(mine0 + r, passes)
        xhat, scale = norm_stats(embed(x, which, table, here))
        da = rd.total(r, RS)
        add_eight(ACC, 0, da * xhat)
        add_eight(ACC, 8, da)
        e = da * gain1
        inner = e - jnp.mean(e, -1, keepdims=True) - xhat * jnp.mean(e * xhat, -1, keepdims=True)
        gi = dh1[here, :] + inner * scale
        gi_o[here, :] = gi
        for p in range(PASSES_MAX):
            add_eight(ACC, 16 + 8 * p, jnp.where(which == p, gi, 0.0))

    over_rows(rows, end_rows)
    VB[0] = jnp.zeros_like(VB[0])
    for n in range(2):
        VB[0, pl.ds(n, 1), :] = jnp.sum(ACC[8 * n : 8 * n + 8, :], 0, keepdims=True)
        VB[0, pl.ds(2 + n, 1), :] = jnp.sum(vec2[8 * n : 8 * n + 8, :], 0, keepdims=True)
    for p in range(PASSES_MAX):
        VB[0, pl.ds(4 + p, 1), :] = jnp.sum(ACC[16 + 8 * p : 24 + 8 * p, :], 0, keepdims=True)
    rounds = []
    for n, other in enumerate(others):
        c = rcopy(VB.at[n], VIN.at[n], sv.at[n], rv.at[n], other)
        c.start()
        if halving and n == 0:
            hq[2].take_two()
        if halving and n == 1:
            gq_o[0] = hq[0].take_three()
        if halving and n == 2:
            gq_o[1] = hq[1].take_three()
        c.wait_recv()
        VB[n + 1] = VB[n] + VIN[n]
        rounds.append(c)
    if halving:
        share = feats // 8
        for k in range(8):

            @pl.when(d == k)
            def _():
                vec_o[...] = VB[len(others), :, k * share : (k + 1) * share]

        gq_o[2] = hq[2].take_three()
        for h in hf + [ht] + hq:
            h.finish_sends()
    else:
        vec_o[...] = VB[len(others)]
    for c in rounds:
        c.wait_send()
    rd.finish_sends()


def backward_call(passes, x, table, g1, h1, dh1, vec2, qc, kc, vc, o, lse, a, zp, wq, wo, gd, gu, halving):
    rows, feats = x.shape
    slots, local = o.shape
    heads = local // HD
    hidden = gd.shape[1]
    ng = 1 + 2 * CHUNKS
    ends = 5 if halving else 2
    share = feats // 8
    cat = vb(heads, slots, 4 * HD)
    wide = vm(heads, slots, 2 * HD)
    outs = [struct(rows, feats), struct(rows, feats), struct(16, share if halving else feats)]
    args = [passes, x, table, g1, h1, dh1, vec2, qc, kc, vc, o, lse, a, zp, wq, wo]
    scratch = [
        cat, cat, cat, cat, vm(heads, 1, slots), vm(heads, 8, QB), vm(slots, feats), vm(heads, QB, 2 * HD), wide, wide, vm(3, slots, local),
        vm(rows, feats), vm(rows, feats), vm(rows, feats), vm(slots, feats), vm(rows, feats), vm(rows, feats), vm(rows, feats),
        vm(3, local, feats), vm(local, feats), vm(16 + 8 * PASSES_MAX, feats), vm(ends + 1, 16, feats), vm(ends, 16, feats),
    ]
    sems = pairs(2, ng, ng, ng, ends) + pairs(1, 25)
    if halving:
        outs += [struct(local, share), struct(3, share, local), struct(share, hidden), struct(share, hidden)]
        args += [gd.reshape(8, share, hidden), gu.reshape(8, share, hidden)]
        scratch += [vm(8, share, local), vm(3, 8, share, local)]
        width = hidden // 2
        scratch += [vm(4, 4, share, width), vm(4, share, local), vm(3, 4, share, local)]
        scratch += [vm(4, 4, share, width), vm(4, 2, share, width), vm(4, share, width)]
        scratch += [vm(4, share, local), vm(2, share, local), vm(share, local)]
        scratch += [vm(3, 4, share, local), vm(3, 2, share, local), vm(3, share, local)]
        sems += pairs(2, 56)
    else:
        outs += [struct(feats, local), struct(3, feats, local)]
    return pl.pallas_call(
        functools.partial(backward_kernel, (rows, slots, feats, heads, CHUNKS, halving)),
        out_shape=tuple(outs),
        in_specs=[IN_SMEM] + [IN_VMEM] * 6 + [IN_HBM] * (len(args) - 7),
        out_specs=(IN_VMEM,) * len(outs),
        scratch_shapes=scratch + sems,
        compiler_params=params(3),
        name="backward_part",
    )(*args)


def per_device(
    block_input, passes, pass_map, pass_table, gain_one, bias_one, w_qkv, w_out, gain_two, bias_two, w_up, w_down, grad_output
):
    x, go = block_input[0], grad_output[0]
    rows, feats = x.shape
    slots = rows * lax.axis_size("tensor")
    ways = lax.axis_size("dp")
    halving = ways == 8
    wq = jnp.transpose(w_qkv, (1, 2, 0))
    a, qc, kc, vc, o, lse, h1, c, dz = forward_call(
        passes, x, pass_table, gain_one, bias_one, gain_two, bias_two, go, wq, w_out, slots
    )
    dh1, vec2, zp, gd, gu = middle_call(h1, go, gain_two, c, dz, w_up, w_down)
    got = backward_call(passes, x, pass_table, gain_one, h1, dh1, vec2, qc, kc, vc, o, lse, a, zp, wq, w_out, gd, gu, halving)
    out, gi, part, gt, gq = got[:5]
    if halving:
        gd, gu = got[5:]
    else:
        gt, gq, gu, gd = (lax.psum_scatter(v, "dp", scatter_dimension=0, tiled=True) for v in (gt, jnp.swapaxes(gq, 0, 1), gu, gd))
        part = lax.psum_scatter(part, "dp", scatter_dimension=1, tiled=True)
        gt, gq = gt.T, jnp.swapaxes(gq, 0, 1)
    return (
        out[None], gi[None], part[4 : 4 + PASSES_MAX], part[0], part[1], jnp.swapaxes(gq, 0, 1), gt, part[2], part[3], gu, gd.T,
    )


def solution(mesh):
    placed = (
        P("dp", "tensor", None), P("dp"), P("dp", "tensor"), P(), P(), P(), P(None, None, "tensor"), P("tensor", None),
        P(), P(), P(None, "tensor"), P("tensor", None), P("dp", "tensor", None),
    )
    return jax.shard_map(
        per_device,
        mesh=mesh,
        in_specs=placed,
        out_specs=(
            P("dp", "tensor", None), P("dp", "tensor", None), P(None, "dp"), P("dp"), P("dp"), P("dp", None, "tensor"),
            P("tensor", "dp"), P("dp"), P("dp"), P("dp", "tensor"), P("tensor", "dp"),
        ),
        check_vma=False,
    )
```

```python
import math
import functools
import jax
import jax.numpy as jnp
from jax import lax
from jax.experimental import pallas as pl
from jax.experimental.pallas import tpu as pltpu
from jax.sharding import PartitionSpec as P

f32 = jnp.float32
bf16 = jnp.bfloat16
HD = 64
BASE = 256
PASSES_MAX = 5
EPSILON = 1e-05
HUGE = 1e30
QB = 256
HIGH = lax.Precision.HIGH
MESH = pl.DeviceIdType.MESH
NN = (((1,), (0,)), ((), ()))
NT = (((1,), (1,)), ((), ()))
TN = (((0,), (0,)), ((), ()))


def mm(left, right, dims=NN):
    return lax.dot_general(left, right, dims, precision=HIGH, preferred_element_type=f32)


def bdot(left, right, dims=NN):
    return lax.dot_general(left, right, dims, preferred_element_type=f32)


def halves(value):
    high = value.astype(bf16)
    return high, (value - high.astype(f32)).astype(bf16)


def rcopy(src, dst, send, recv, where):
    return pltpu.make_async_remote_copy(
        src_ref=src, dst_ref=dst, send_sem=send, recv_sem=recv, device_id=where, device_id_type=MESH
    )


def places():
    t = lax.axis_index("tensor")
    sib = t + 1 - 2 * (t % 2)
    yp = (t + 2) % 4
    far = (sib + 2) % 4
    return t, sib, yp, far


def greet(others):
    for other in others:
        pl.semaphore_signal(pltpu.get_barrier_semaphore(), inc=1, device_id=other, device_id_type=MESH)


def met(others):
    pl.semaphore_wait(pltpu.get_barrier_semaphore(), len(others))


def order_of(n, owners):
    out = owners[0]
    for k in range(1, len(owners)):
        here = (n + len(owners) - k) // len(owners) - (n + len(owners) - k - 1) // len(owners)
        out = out + here * (owners[k] - owners[0])
    return out


def block(owner, rows, chunk=0, chunks=1):
    size = rows // chunks
    return pl.ds(pl.multiple_of(owner * rows + chunk * size, 8), size)


class Gather:
    def __init__(self, buf, send, recv, rows, chunks, source=None):
        t, sib, yp, far = places()
        self.own, self.yp, self.sib, self.far, self.rows, self.chunks = t, yp, sib, far, rows, chunks
        self.across, self.fwd = [], []
        mine = buf.at[block(t, rows)]
        self.side = rcopy(mine if source is None else source, mine, send.at[0], recv.at[0], {"tensor": sib})
        for k in range(chunks):
            part = buf.at[block(t, rows, k, chunks)]
            first = part if source is None else source.at[pl.ds(k * (rows // chunks), rows // chunks)]
            self.across.append(rcopy(first, part, send.at[1 + k], recv.at[1 + k], {"tensor": yp}))
            part = buf.at[block(yp, rows, k, chunks)]
            j = 1 + chunks + k
            self.fwd.append(rcopy(part, part, send.at[j], recv.at[j], {"tensor": sib}))

    def start(self):
        for c in self.across:
            c.start()
        self.side.start()

    def relay(self, k):
        self.across[k].wait_recv()
        self.fwd[k].start()

    def finish_sends(self):
        self.side.wait_send()
        for c in self.across + self.fwd:
            c.wait_send()


class Scatter:
    def __init__(self, part, own_in, pre_in, y_in, send, recv, rows, chunks):
        t, sib, yp, far = places()
        self.part, self.own_in, self.pre_in, self.y_in = part, own_in, pre_in, y_in
        self.rows, self.chunks, self.size = rows, chunks, rows // chunks
        self.t, self.sib, self.yp, self.far = t, sib, yp, far
        self.side = rcopy(part.at[block(sib, rows)], own_in, send.at[0], recv.at[0], {"tensor": sib})
        self.pre, self.across = [], []
        for k in range(chunks):
            here = pl.ds(k * self.size, self.size)
            self.pre.append(
                rcopy(part.at[block(far, rows, k, chunks)], pre_in.at[here], send.at[1 + k], recv.at[1 + k], {"tensor": sib})
            )
            j = 1 + chunks + k
            self.across.append(rcopy(pre_in.at[here], y_in.at[here], send.at[j], recv.at[j], {"tensor": yp}))

    def send_pre(self, k):
        self.pre[k].start()

    def send_across(self, k):
        self.pre[k].wait_recv()
        here = pl.ds(k * self.size, self.size)
        self.pre_in[here, :] = self.part[block(self.yp, self.rows, k, self.chunks), :] + self.pre_in[here, :]
        self.across[k].start()

    def send_side(self):
        self.side.start()

    def arrive(self):
        self.side.wait_recv()
        for c in self.across:
            c.wait_recv()

    def total(self, start, size):
        here = pl.ds(start, size)
        mine = pl.ds(pl.multiple_of(self.t * self.rows + start, 8), size)
        return self.part[mine, :] + self.own_in[here, :] + self.y_in[here, :]

    def finish_sends(self):
        self.side.wait_send()
        for c in self.pre + self.across:
            c.wait_send()


def slot_facts(start, passes_ref):
    count = passes_ref[0]
    slot = start + lax.broadcasted_iota(jnp.int32, (RS, 1), 0)
    which = jnp.zeros_like(slot)
    for r in range(1, PASSES_MAX + 1):
        which = jnp.where(count == r, slot % r, which)
    return which, jnp.where(slot < count * BASE, 1.0, 0.0)


def embed(x_ref, which, table_ref, here):
    rows = x_ref[here, :]
    added = jnp.zeros_like(rows)
    for p in range(PASSES_MAX):
        added = jnp.where(which == p, table_ref[pl.ds(p, 1), :], added)
    return rows + added


def norm_stats(values):
    center = values - jnp.mean(values, -1, keepdims=True)
    spread = jnp.mean(center * center, -1, keepdims=True)
    scale = lax.rsqrt(spread + EPSILON)
    return center * scale, scale


RS = 32


def over_rows(rows, body, size=RS):
    def step(i, carry):
        body(pl.multiple_of(i * size, size))
        return carry

    lax.fori_loop(0, rows // size, step, 0)


def cat_q(v):
    high = v.astype(bf16).astype(f32)
    low = v - high
    return jnp.concatenate([high, low, low, high], axis=1).astype(bf16)


def cat_k(v):
    high = v.astype(bf16).astype(f32)
    low = v - high
    return jnp.concatenate([high, low, high, low], axis=1).astype(bf16)


def fold(both):
    return both[:, :HD] + both[:, HD:]


def causal(s, size):
    row = lax.broadcasted_iota(jnp.int32, (QB, QB), 0)
    col = lax.broadcasted_iota(jnp.int32, (QB, QB), 1)
    last = jnp.where(col <= row, s[:, size - QB :], -HUGE)
    return last if size == QB else jnp.concatenate([s[:, : size - QB], last], axis=1)


def add_eight(ref, row, value):
    total = value[0:8, :]
    for k in range(1, value.shape[0] // 8):
        total = total + value[8 * k : 8 * k + 8, :]
    ref[pl.ds(row, 8), :] = ref[pl.ds(row, 8), :] + total


def row_of(ref):
    return ref[...].reshape(1, ref.shape[0])


def forward_kernel(
    dims, passes, x, table, g1, b1, g2, b2, go, wq_h, wo_h,
    a_o, qc_o, kc_o, vc_o, o_o, lse_o, h1_o, c_o, dz_o,
    A, DZ, QC, KC, VC, O, LSE, TOP, SUM, OT, PT, OWN, PRE, YIN, WQ, WO,
    s1, r1, s2, r2, s3, r3, ls,
):
    rows, slots, feats, heads, chunks = dims
    t, sib, yp, far = places()
    mine0 = t * rows
    loads = [pltpu.make_async_copy(wq_h, WQ, ls.at[0]), pltpu.make_async_copy(wo_h, WO, ls.at[1])]
    for c in loads:
        c.start()
    gain, bias = row_of(g1), row_of(b1)

    others = [{"tensor": sib}, {"tensor": yp}]
    greet(others)
    ga = Gather(A, s1, r1, rows, chunks)
    gz = Gather(DZ, s2, r2, rows, chunks)

    def begin_rows(r):
        here = pl.ds(r, RS)
        which, _ = slot_facts(mine0 + r, passes)
        h0 = embed(x, which, table, here)
        h1_o[here, :] = h0
        xhat, _ = norm_stats(h0)
        A[pl.ds(pl.multiple_of(mine0 + r, RS), RS), :] = xhat * gain + bias

    over_rows(rows // 2, begin_rows)
    met(others)
    ga.across[0].start()
    over_rows(rows // 2, lambda r: begin_rows(r + rows // 2))
    ga.across[1].start()
    ga.side.start()

    def mask_rows(r):
        here = pl.ds(r, RS)
        _, live = slot_facts(mine0 + r, passes)
        DZ[pl.ds(pl.multiple_of(mine0 + r, RS), RS), :] = live * go[here, :]

    over_rows(rows, mask_rows)
    loads[0].wait()
    outs = []

    def project(n, carry):
        @pl.when(n == 1)
        def _():
            ga.side.wait_recv()

        @pl.when(n == 2)
        def _():
            for k in range(chunks):
                ga.relay(k)
            gz.start()

        @pl.when(n == 3)
        def _():
            for k in range(chunks):
                ga.fwd[k].wait_recv()

        here = block(order_of(n, (t, sib, yp, far)), rows)
        for c, (ref, cat) in enumerate(((QC, cat_q), (KC, cat_k), (VC, cat_k))):
            pr = mm(A[here, :], WQ[c], NT)
            if c == 0:
                pr = pr * (1.0 / math.sqrt(HD))
            for h in range(heads):
                ref[h, here, :] = cat(pr[:, h * HD : (h + 1) * HD])
        return carry

    lax.fori_loop(0, 4, project, 0)
    more = [
        pltpu.make_async_copy(A, a_o, ls.at[3]),
        pltpu.make_async_copy(QC, qc_o, ls.at[4]),
        pltpu.make_async_copy(KC, kc_o, ls.at[5]),
        pltpu.make_async_copy(VC, vc_o, ls.at[6]),
    ]
    for c in more:
        c.start()
    outs += more
    loads[1].wait()
    blocks = slots // QB
    row = lax.broadcasted_iota(jnp.int32, (QB, QB), 0)
    col = lax.broadcasted_iota(jnp.int32, (QB, QB), 1)
    upper = t // 2
    rs = Scatter(PT, OWN, PRE, YIN, s3, r3, rows, chunks)

    def attend(n, carry):
        i = upper * n + (1 - upper) * (blocks - 1 - n)
        q_rows = pl.ds(pl.multiple_of(i * QB, QB), QB)
        TOP[...] = jnp.full(TOP.shape, -HUGE, f32)
        SUM[...] = jnp.zeros(SUM.shape, f32)
        OT[...] = jnp.zeros(OT.shape, f32)

        def keys(j, inner):
            k_rows = pl.ds(pl.multiple_of(j * QB, QB), QB)
            ok = (row <= col) | (j < i)
            for h in range(heads):
                s = jnp.where(ok, bdot(KC[h, k_rows, :], QC[h, q_rows, :], NT), -HUGE)
                old = TOP[h]
                new = jnp.maximum(old, jnp.max(s, 0, keepdims=True))
                shrink = jnp.exp(old - new)
                p = jnp.exp(s - new)
                TOP[h] = new
                SUM[h] = SUM[h] * shrink + jnp.sum(p, 0, keepdims=True)
                ph, pw = halves(p)
                values = VC[h, k_rows, 0 : 2 * HD]
                OT[h] = OT[h] * shrink + (bdot(values, ph, TN) + bdot(values, pw, TN))
            return inner

        lax.fori_loop(0, i + 1, keys, 0)
        parts = []
        for h in range(heads):
            parts.append((OT[h, :HD, :] + OT[h, HD:, :]) / SUM[h])
            LSE[h, :, q_rows] = TOP[h] + jnp.log(SUM[h])
        o = jnp.concatenate(parts, axis=0).T
        O[q_rows, :] = o
        PT[q_rows, :] = mm(o, WO[...])

        @pl.when(n == 2)
        def _():
            for k in range(chunks):
                rs.send_pre(k)

        @pl.when(n == 3)
        def _():
            for k in range(chunks):
                rs.send_across(k)
            gz.side.wait_recv()

        return carry

    lax.fori_loop(0, blocks, attend, 0)
    rs.send_side()
    for k in range(chunks):
        gz.relay(k)
    more = [pltpu.make_async_copy(O, o_o, ls.at[7]), pltpu.make_async_copy(LSE, lse_o, ls.at[8])]
    for c in more:
        c.start()
    outs += more
    for k in range(chunks):
        gz.fwd[k].wait_recv()
    more = [pltpu.make_async_copy(DZ, dz_o, ls.at[9])]
    more[0].start()
    outs += more
    rs.arrive()
    gain2, bias2 = row_of(g2), row_of(b2)

    def end_rows(r):
        here = pl.ds(r, RS)
        _, live = slot_facts(mine0 + r, passes)
        h1 = h1_o[here, :] + live * rs.total(r, RS)
        h1_o[here, :] = h1
        xhat, _ = norm_stats(h1)
        c_o[here, :] = xhat * gain2 + bias2

    over_rows(rows, end_rows)
    for c in outs:
        c.wait()
    ga.finish_sends()
    gz.finish_sends()
    rs.finish_sends()


def struct(*shape):
    return jax.ShapeDtypeStruct(shape, f32)


def vm(*shape):
    return pltpu.VMEM(shape, f32)


def vb(*shape):
    return pltpu.VMEM(shape, bf16)


def pairs(count, *numbers):
    return [pltpu.SemaphoreType.DMA((n,)) for n in numbers for _ in range(count)]


IN_VMEM = pl.BlockSpec(memory_space=pltpu.VMEM)
IN_SMEM = pl.BlockSpec(memory_space=pltpu.SMEM)
IN_HBM = pl.BlockSpec(memory_space=pl.ANY)
CHUNKS = 2


def params(number):
    return pltpu.CompilerParams(collective_id=number, has_side_effects=True, vmem_limit_bytes=63 << 20)


def forward_call(passes, x, table, g1, b1, g2, b2, go, wq, wo, slots):
    rows, feats = x.shape
    local = wq.shape[1]
    heads = local // HD
    cat = jax.ShapeDtypeStruct((heads, slots, 4 * HD), bf16)
    ng = 1 + 2 * CHUNKS
    return pl.pallas_call(
        functools.partial(forward_kernel, (rows, slots, feats, heads, CHUNKS)),
        out_shape=(
            struct(slots, feats), cat, cat, cat, struct(slots, local), struct(heads, 1, slots),
            struct(rows, feats), struct(rows, feats), struct(slots, feats),
        ),
        in_specs=[IN_SMEM] + [IN_VMEM] * 7 + [IN_HBM] * 2,
        out_specs=(IN_HBM,) * 6 + (IN_VMEM, IN_VMEM, IN_HBM),
        scratch_shapes=[
            vm(slots, feats), vm(slots, feats),
            vb(heads, slots, 4 * HD), vb(heads, slots, 4 * HD), vb(heads, slots, 4 * HD),
            vm(slots, local), vm(heads, 1, slots), vm(heads, 1, QB), vm(heads, 1, QB), vm(heads, 2 * HD, QB), vm(slots, feats),
            vm(rows, feats), vm(rows, feats), vm(rows, feats),
            vm(3, local, feats), vm(local, feats),
        ] + pairs(2, ng, ng, ng) + pairs(1, 10),
        compiler_params=params(1),
        name="forward_part",
    )(passes, x, table, g1, b1, g2, b2, go, wq, wo)


FF_ORDERS = ((0, 1, 2), (1, 2, 0), (0, 1, 2), (0, 1, 2))
Q_ORDERS = ((0, 1, 2), (1, 0, 2), (0, 1, 2))


class Halve:
    def __init__(self, source, keep, in_one, in_two, in_three, send, recv, base, order):
        d = lax.axis_index("dp")
        bits = (d % 2, (d // 2) % 2, d // 4)
        peers = ({"dp": d + 1 - 2 * bits[0]}, {"dp": d + 2 - 4 * bits[1]}, {"dp": (d + 4) % 8})
        a1, a2, a3 = order
        self.mid, self.last = bits[a2], bits[a3]
        self.spot = (lambda x, y: 2 * x + y) if a2 > a3 else (lambda x, y: 2 * y + x)
        self.keep, self.ins = keep, (in_one, in_two, in_three)

        def whole(v, x, y):
            return v * 2**a1 + x * 2**a2 + y * 2**a3

        pick = [(x, y) for x in range(2) for y in range(2)]
        self.own = [(whole(bits[a1], x, y), self.spot(x, y)) for x, y in pick]
        self.one = [
            rcopy(source.at[whole(1 - bits[a1], x, y)], in_one.at[self.spot(x, y)], send.at[base + n], recv.at[base + n], peers[a1])
            for n, (x, y) in enumerate(pick)
        ]
        if in_two is None:
            return
        self.two = [
            rcopy(keep.at[self.spot(1 - self.mid, y)], in_two.at[y], send.at[base + 4 + y], recv.at[base + 4 + y], peers[a2])
            for y in range(2)
        ]
        self.three = rcopy(keep.at[self.spot(self.mid, 1 - self.last)], in_three, send.at[base + 6], recv.at[base + 6], peers[a3])

    def start_one(self):
        for c in self.one:
            c.start()

    def add_one(self):
        for c in self.one:
            c.wait_recv()
        self.keep[...] = self.keep[...] + self.ins[0][...]

    def start_two(self):
        for c in self.two:
            c.start()

    def take_one(self):
        self.add_one()
        self.start_two()

    def take_two(self):
        for y in range(2):
            self.two[y].wait_recv()
            at = self.spot(self.mid, y)
            self.keep[at] = self.keep[at] + self.ins[1][y]
        self.three.start()

    def take_three(self):
        self.three.wait_recv()
        return self.keep[self.spot(self.mid, self.last)] + self.ins[2][...]

    def finish_sends(self, first=True):
        for c in (self.one if first else []) + self.two + [self.three]:
            c.wait_send()


def gelu_both(u):
    k = math.sqrt(2.0 / math.pi)
    square = u * u
    th = jnp.tanh(k * (u * (1.0 + 0.044715 * square)))
    half = 0.5 * (1.0 + th)
    slope = half + (0.5 * k) * u * (1.0 - th * th) * (1.0 + (3.0 * 0.044715) * square)
    return u * half, slope


def middle_kernel(dims, *refs):
    rows, slots, feats, chunks, halving = dims
    refs = list(refs)

    def take(n):
        out = refs[:n]
        del refs[:n]
        return out

    h1, go, g2, c_h, dz_h, wu_h, wd_h = take(7)
    dh1_o, vec_o, zp_o, gd_o, gu_o = take(5)
    C, DZ, ACT, DU, PT, OWN, PRE, YIN, WU, WD, GD, GU = take(12)
    if halving:
        KG, G1 = take(2)
    s1, r1, s2, r2, ls = take(5)
    if halving:
        sh, rh = take(2)
    t, sib, yp, far = places()
    first = pltpu.make_async_copy(c_h, C.at[block(t, rows)], ls.at[0])
    loads = [
        pltpu.make_async_copy(wd_h, WD, ls.at[1]),
        pltpu.make_async_copy(dz_h, DZ, ls.at[2]),
        pltpu.make_async_copy(wu_h, WU, ls.at[3]),
    ]
    first.start()
    for c in loads:
        c.start()
    others = [{"tensor": sib}, {"tensor": yp}]
    if halving:
        d = lax.axis_index("dp")
        others += [{"dp": d + 1 - 2 * (d % 2)}, {"dp": d + 2 - 4 * ((d // 2) % 2)}]
    greet(others)
    gc = Gather(C, s1, r1, rows, chunks, c_h)
    met(others)
    gc.start()
    first.wait()
    for c in loads:
        c.wait()

    def open_block(i, carry):
        here = block(i, rows)
        DU[here, :] = mm(DZ[here, :], WD[...], NT)
        return carry

    lax.fori_loop(0, slots // rows, open_block, 0)

    def work(here):
        act, slope = gelu_both(mm(C[here, :], WU[...]))
        ACT[here, :] = act
        du = DU[here, :] * slope
        DU[here, :] = du
        PT[here, :] = mm(du, WU[...], NT)

    rs = Scatter(PT, OWN, PRE, YIN, s2, r2, rows, chunks)

    def step(n, carry):
        @pl.when(n == 2)
        def _():
            gc.side.wait_recv()

        for k in range(chunks):

            @pl.when(n == 4 + 2 * k)
            def _():
                gc.relay(k)
                gc.fwd[k].wait_recv()

        late = n // 4
        k = late * ((n % 4) // 2) + (1 - late) * (n % 2)
        owner = late * ((n % 2) * yp + (1 - n % 2) * far) + (1 - late) * ((n // 2) * sib + (1 - n // 2) * t)
        here = pl.ds(pl.multiple_of(owner * rows + k * (rows // chunks), 8), rows // chunks)
        act, slope = gelu_both(mm(C[here, :], WU[...]))
        ACT[here, :] = act
        du = DU[here, :] * slope
        DU[here, :] = du
        PT[here, :] = mm(du, WU[...], NT)

        @pl.when(n == 3)
        def _():
            rs.send_side()

        for k in range(chunks):

            @pl.when(n == 4 + 2 * k)
            def _():
                rs.send_pre(k)

            @pl.when(n == 5 + 2 * k)
            def _():
                rs.send_across(k)

        return carry

    lax.fori_loop(0, 4 + 2 * chunks, step, 0)

    def grads(left, right, out):
        def step(n, carry):
            cols = pl.ds(pl.multiple_of(n * (feats // 2), 128), feats // 2)
            out[pl.ds(4 * n, 4)] = mm(left[:, cols], right[...], TN).reshape(4, feats // 8, feats)
            return carry

        lax.fori_loop(0, 2, step, 0)

    grads(C, DU, GU)
    if halving:
        width = KG.shape[-1]
        hg = []
        for n in range(2):
            half = GU.at[:, :, pl.ds(n * width, width)]
            hg.append(Halve(half, KG.at[n], G1.at[n], None, None, sh, rh, 4 * n, FF_ORDERS[n]))
            hg[n].start_one()
        for n in range(2):
            for a, b in hg[n].own:
                KG[n, b] = GU[a, :, n * width : (n + 1) * width]
    else:
        gu_copy = pltpu.make_async_copy(GU, gu_o, ls.at[4])
        gu_copy.start()
    grads(DZ, ACT, GD)
    gd_copy = pltpu.make_async_copy(GD, gd_o, ls.at[5])
    gd_copy.start()

    def down(i, carry):
        here = block(i, rows)
        DZ[here, :] = mm(ACT[here, :], WD[...])
        return carry

    lax.fori_loop(0, slots // rows, down, 0)
    zp_copy = pltpu.make_async_copy(DZ, zp_o, ls.at[6])
    zp_copy.start()
    vec_o[...] = jnp.zeros_like(vec_o)
    gain2 = row_of(g2)
    rs.arrive()

    def end_rows(r):
        here = pl.ds(r, RS)
        dc = rs.total(r, RS)
        xhat, scale = norm_stats(h1[here, :])
        add_eight(vec_o, 0, dc * xhat)
        add_eight(vec_o, 8, dc)
        e = dc * gain2
        inner = e - jnp.mean(e, -1, keepdims=True) - xhat * jnp.mean(e * xhat, -1, keepdims=True)
        dh1_o[here, :] = go[here, :] + inner * scale

    over_rows(rows, end_rows)
    if halving:
        for h in hg:
            h.add_one()
        gu_copy = pltpu.make_async_copy(KG, gu_o, ls.at[4])
        gu_copy.start()
        for h in hg:
            for c in h.one:
                c.wait_send()
    for c in (gu_copy, gd_copy, zp_copy):
        c.wait()
    gc.finish_sends()
    rs.finish_sends()


def middle_call(h1, go, g2, c, dz, wu, wd, halving):
    rows, feats = h1.shape
    slots = dz.shape[0]
    hidden = wu.shape[1]
    ng = 1 + 2 * CHUNKS
    share = feats // 8
    part = (2, 4, share, hidden // 2)
    grad = (8, share, hidden)
    return pl.pallas_call(
        functools.partial(middle_kernel, (rows, slots, feats, CHUNKS, halving)),
        out_shape=(
            struct(rows, feats), struct(16, feats), struct(slots, feats), struct(*grad), struct(*(part if halving else grad)),
        ),
        in_specs=[IN_VMEM] * 3 + [IN_HBM] * 4,
        out_specs=(IN_VMEM, IN_VMEM, IN_HBM, IN_HBM, IN_HBM),
        scratch_shapes=[
            vm(slots, feats), vm(slots, feats), vm(slots, hidden), vm(slots, hidden), vm(slots, feats),
            vm(rows, feats), vm(rows, feats), vm(rows, feats),
            vm(feats, hidden), vm(hidden, feats), vm(*grad), vm(*grad),
        ] + ([vm(*part), vm(*part)] if halving else []) + pairs(2, ng, ng) + pairs(1, 7) + (pairs(2, 8) if halving else []),
        compiler_params=params(2),
        name="middle_part",
    )(h1, go, g2, c, dz, wu, wd)


def backward_kernel(dims, *refs):
    rows, slots, feats, heads, chunks, halving = dims
    refs = list(refs)

    def take(n):
        out = refs[:n]
        del refs[:n]
        return out

    passes, x, table, g1, h1, dh1, vec2 = take(7)
    qc_h, kc_h, vc_h, o_h, lse_h, a_h, zp_h, wq_h, wo_h = take(9)
    if halving:
        gd_h, gu_h = take(2)
    out_o, gi_o, vec_o, gt_o, gq_o = take(5)
    if halving:
        gd_o, gu_o = take(2)
    QC, KC, VC, DOC, LSE, DROW, DATT, DQ, DK, DV, DP = take(11)
    OWN, PRE, YIN, ZP, ZOWN, ZPRE, ZYIN, WQ, WO, ACC, VB, VIN = take(12)
    if halving:
        GT, GQ, KF, KT, KQ, F1, F2, F3, T1, T2, T3, Q1, Q2, Q3 = take(14)
    s1, r1, s2, r2, s3, r3, sv, rv, ls = take(9)
    if halving:
        sh, rh = take(2)
    O = DP.at[0]
    t, sib, yp, far = places()
    mine0 = t * rows
    loads = [
        pltpu.make_async_copy(src, dst, ls.at[n])
        for n, (src, dst) in enumerate(
            ((wo_h, WO), (o_h, DP.at[0]), (zp_h, ZP), (qc_h, QC), (kc_h, KC), (vc_h, VC), (lse_h, LSE), (wq_h, WQ))
        )
    ]
    if halving:
        d = lax.axis_index("dp")
        low = d % 2
        width = KF.shape[-1]
        hf = []
        for n in range(4):
            ref = gd_h.at[:, :, pl.ds(n % 2 * width, width)]
            hf.append(Halve(ref, KF.at[n], F1.at[n // 2 * (n - 2)], F2.at[n], F3.at[n], sh, rh, 7 * n, FF_ORDERS[n]))
        loads += [pltpu.make_async_copy(gu_h.at[n], KF.at[n], ls.at[9 + n]) for n in range(2)]
        for n in (2, 3):
            ref = gd_h.at[:, :, pl.ds(n % 2 * width, width)]
            loads += [
                pltpu.make_async_copy(ref.at[a], KF.at[n, b], ls.at[3 + 4 * n + m]) for m, (a, b) in enumerate(hf[n].own)
            ]
        early = loads[8:]
    for c in loads:
        c.start()

    others = [{"tensor": sib}, {"tensor": yp}]
    if halving:
        others += [{"dp": d + 1 - 2 * low}, {"dp": d + 2 - 4 * ((d // 2) % 2)}, {"dp": (d + 4) % 8}]
    greet(others)

    def begin_rows(r):
        here = pl.ds(r, RS)
        _, live = slot_facts(mine0 + r, passes)
        DATT[pl.ds(pl.multiple_of(mine0 + r, RS), RS), :] = live * dh1[here, :]

    over_rows(rows, begin_rows)
    met(others)
    gt = Gather(DATT, s1, r1, rows, chunks)
    gt.start()
    if halving:
        for n in (2, 3):
            hf[n].start_one()
        for c in early[:2]:
            c.wait()
        hf[0].start_two()
        hf[1].start_two()
        base = 28
        ht = Halve(GT, KT, T1, T2, T3, sh, rh, base, (0, 1, 2))
        hq = [Halve(GQ.at[c], KQ.at[c], Q1.at[c], Q2.at[c], Q3.at[c], sh, rh, base + 7 + 7 * c, Q_ORDERS[c]) for c in range(3)]

        def ff_out(n):
            k = n % 2
            if n < 2:
                gu_o[:, k * width : (k + 1) * width] = hf[n].take_three()
            else:
                gd_o[:, k * width : (k + 1) * width] = hf[n].take_three()
    rz = Scatter(ZP, ZOWN, ZPRE, ZYIN, s2, r2, rows, chunks)
    loads[2].wait()
    for k in range(chunks):
        rz.send_pre(k)
    rz.send_side()
    loads[0].wait()

    def mixed_grad(n, carry):
        @pl.when(n == 1)
        def _():
            gt.side.wait_recv()

        @pl.when(n == 2)
        def _():
            for k in range(chunks):
                gt.relay(k)
            for k in range(chunks):
                rz.send_across(k)
            if halving:
                for c in early[2:]:
                    c.wait()
                hf[0].take_two()
                hf[1].take_two()
                hf[2].take_one()

        @pl.when(n == 3)
        def _():
            for k in range(chunks):
                gt.fwd[k].wait_recv()

        here = block(order_of(n, (t, sib, yp, far)), rows)
        do = mm(DATT[here, :], WO[...], NT)
        for h in range(heads):
            DOC[h, here, :] = cat_q(do[:, h * HD : (h + 1) * HD])
        return carry

    lax.fori_loop(0, 4, mixed_grad, 0)
    loads[1].wait()
    grad_out = mm(DATT[...], O[...], TN)
    for c in loads[3:8]:
        c.wait()
    if halving:
        GT[...] = grad_out.reshape(GT.shape)
        for a, b in ht.own:
            KT[b] = GT[a]
        ht.start_one()
    else:
        gt_o[...] = grad_out
    gt.finish_sends()
    blocks = slots // QB
    row = lax.broadcasted_iota(jnp.int32, (QB, QB), 0)
    col = lax.broadcasted_iota(jnp.int32, (QB, QB), 1)
    ones = jnp.ones((8, HD), f32)
    for i in reversed(range(blocks)):
        q_rows = pl.ds(i * QB, QB)
        size = (i + 1) * QB
        k_rows = pl.ds(0, size)
        for h in range(heads):
            do = fold(DOC[h, q_rows, 0 : 2 * HD].astype(f32))
            DROW[h] = mm(ones, do * O[q_rows, h * HD : (h + 1) * HD], NT)

        def one_head(h, carry):
            q, do = QC[h, q_rows, :], DOC[h, q_rows, :]
            s = bdot(KC[h, k_rows, :], q, NT)
            last = jnp.where(row <= col, s[size - QB :, :], -HUGE)
            s = last if i == 0 else jnp.concatenate([s[: size - QB, :], last], axis=0)
            p = jnp.exp(s - LSE[h, :, q_rows])
            ds = p * (bdot(VC[h, k_rows, :], do, NT) - DROW[h, 0:1, :])
            ph, pw = halves(p)
            dsh, dsw = halves(ds)
            do2, q2 = do[:, : 2 * HD], q[:, : 2 * HD]
            dv = bdot(ph, do2) + bdot(pw, do2)
            dk = bdot(dsh, q2) + bdot(dsw, q2)
            keys = KC[h, k_rows, 0 : 2 * HD]
            DQ[h, :, :] = bdot(dsh, keys, TN) + bdot(dsw, keys, TN)
            if i == blocks - 1:
                DV[h, :, :] = dv
                DK[h, :, :] = dk
            else:
                DV[h, k_rows, :] = DV[h, k_rows, :] + dv
                DK[h, k_rows, :] = DK[h, k_rows, :] + dk
            return carry

        lax.fori_loop(0, heads, one_head, 0)
        dq = jnp.concatenate([fold(DQ[h]) for h in range(heads)], axis=1)
        DP[0, q_rows, :] = dq * (1.0 / math.sqrt(HD))
        if halving and i == 4:
            ff_out(0)
            hf[3].take_one()
        if halving and i == 3:
            hf[2].take_two()
            ff_out(1)
        if halving and i == 2:
            ht.take_one()
        if halving and i == 1:
            hf[3].take_two()
            ff_out(2)
        if halving and i == 0:
            ht.take_two()
    rd = Scatter(DATT, OWN, PRE, YIN, s3, r3, rows, chunks)

    rz.arrive()

    def out_rows(r):
        here = pl.ds(r, RS)
        _, live = slot_facts(mine0 + r, passes)
        out_o[here, :] = h1[here, :] + live * rz.total(r, RS)

    over_rows(rows, out_rows)
    rz.finish_sends()
    a_copy = pltpu.make_async_copy(a_h, ZP, ls.at[8])
    a_copy.start()

    def gather_heads(n, carry):
        here = block(n, rows)
        for c, ref in ((1, DK), (2, DV)):
            DP[c, here, :] = jnp.concatenate([fold(ref[h, here, :]) for h in range(heads)], axis=1)
        return carry

    lax.fori_loop(0, 4, gather_heads, 0)

    def head_grads(n, carry):
        here = block(order_of(n, (far, yp, sib, t)), rows)
        DATT[here, :] = mm(DP[0, here, :], WQ[0]) + mm(DP[1, here, :], WQ[1]) + mm(DP[2, here, :], WQ[2])

        @pl.when(n == 0)
        def _():
            for k in range(chunks):
                rd.send_pre(k)

        @pl.when(n == 1)
        def _():
            for k in range(chunks):
                rd.send_across(k)

        @pl.when(n == 2)
        def _():
            rd.send_side()

        return carry

    lax.fori_loop(0, 2, head_grads, 0)
    a_copy.wait()

    def weight_grads(c, carry):
        full = mm(ZP[...], DP[c], TN)
        if not halving:
            gq_o[c] = full
            return carry
        GQ[c] = full.reshape(GQ.shape[1:])
        for k in range(3):

            @pl.when(c == k)
            def _():
                for a, b in hq[k].own:
                    KQ[k, b] = GQ[k, a]
                hq[k].start_one()

        return carry

    lax.fori_loop(0, 3, weight_grads, 0)
    lax.fori_loop(2, 4, head_grads, 0)
    if halving:
        ff_out(3)
        hq[1].take_one()
        hq[0].take_one()
        hq[1].take_two()
        hq[0].take_two()
        hq[2].take_one()
    ACC[...] = jnp.zeros_like(ACC)
    gain1 = row_of(g1)
    rd.arrive()

    def end_rows(r):
        here = pl.ds(r, RS)
        which, _ = slot_facts(mine0 + r, passes)
        xhat, scale = norm_stats(embed(x, which, table, here))
        da = rd.total(r, RS)
        add_eight(ACC, 0, da * xhat)
        add_eight(ACC, 8, da)
        e = da * gain1
        inner = e - jnp.mean(e, -1, keepdims=True) - xhat * jnp.mean(e * xhat, -1, keepdims=True)
        gi = dh1[here, :] + inner * scale
        gi_o[here, :] = gi
        for p in range(PASSES_MAX):
            add_eight(ACC, 16 + 8 * p, jnp.where(which == p, gi, 0.0))

    over_rows(rows, end_rows)
    VB[0] = jnp.zeros_like(VB[0])
    for n in range(2):
        VB[0, pl.ds(n, 1), :] = jnp.sum(ACC[8 * n : 8 * n + 8, :], 0, keepdims=True)
        VB[0, pl.ds(2 + n, 1), :] = jnp.sum(vec2[8 * n : 8 * n + 8, :], 0, keepdims=True)
    for p in range(PASSES_MAX):
        VB[0, pl.ds(4 + p, 1), :] = jnp.sum(ACC[16 + 8 * p : 24 + 8 * p, :], 0, keepdims=True)
    rounds = []
    for n, other in enumerate(others):
        c = rcopy(VB.at[n], VIN.at[n], sv.at[n], rv.at[n], other)
        c.start()
        if halving and n == 0:
            hq[2].take_two()
            gt_o[...] = ht.take_three().T
        if halving and n == 1:
            gq_o[0] = hq[0].take_three()
        if halving and n == 2:
            gq_o[1] = hq[1].take_three()
        c.wait_recv()
        VB[n + 1] = VB[n] + VIN[n]
        rounds.append(c)
    if halving:
        share = feats // 8
        for k in range(8):

            @pl.when(d == k)
            def _():
                vec_o[...] = VB[len(others), :, k * share : (k + 1) * share]

        gq_o[2] = hq[2].take_three()
        for n, h in enumerate(hf + [ht] + hq):
            h.finish_sends(n >= 2)
    else:
        vec_o[...] = VB[len(others)]
    for c in rounds:
        c.wait_send()
    rd.finish_sends()


def backward_call(passes, x, table, g1, h1, dh1, vec2, qc, kc, vc, o, lse, a, zp, wq, wo, gd, gu, halving):
    rows, feats = x.shape
    slots, local = o.shape
    heads = local // HD
    hidden = gd.shape[2]
    ng = 1 + 2 * CHUNKS
    ends = 5 if halving else 2
    share = feats // 8
    cat = vb(heads, slots, 4 * HD)
    wide = vm(heads, slots, 2 * HD)
    outs = [struct(rows, feats), struct(rows, feats), struct(16, share if halving else feats)]
    args = [passes, x, table, g1, h1, dh1, vec2, qc, kc, vc, o, lse, a, zp, wq, wo]
    scratch = [
        cat, cat, cat, cat, vm(heads, 1, slots), vm(heads, 8, QB), vm(slots, feats), vm(heads, QB, 2 * HD), wide, wide, vm(3, slots, local),
        vm(rows, feats), vm(rows, feats), vm(rows, feats), vm(slots, feats), vm(rows, feats), vm(rows, feats), vm(rows, feats),
        vm(3, local, feats), vm(local, feats), vm(16 + 8 * PASSES_MAX, feats), vm(ends + 1, 16, feats), vm(ends, 16, feats),
    ]
    sems = pairs(2, ng, ng, ng, ends) + pairs(1, 25)
    if halving:
        outs += [struct(local, share), struct(3, share, local), struct(share, hidden), struct(share, hidden)]
        args += [gd, gu]
        scratch += [vm(8, share, local), vm(3, 8, share, local)]
        width = hidden // 2
        scratch += [vm(4, 4, share, width), vm(4, share, local), vm(3, 4, share, local)]
        scratch += [vm(2, 4, share, width), vm(4, 2, share, width), vm(4, share, width)]
        scratch += [vm(4, share, local), vm(2, share, local), vm(share, local)]
        scratch += [vm(3, 4, share, local), vm(3, 2, share, local), vm(3, share, local)]
        sems += pairs(2, 56)
    else:
        outs += [struct(feats, local), struct(3, feats, local)]
    return pl.pallas_call(
        functools.partial(backward_kernel, (rows, slots, feats, heads, CHUNKS, halving)),
        out_shape=tuple(outs),
        in_specs=[IN_SMEM] + [IN_VMEM] * 6 + [IN_HBM] * (len(args) - 7),
        out_specs=(IN_VMEM,) * len(outs),
        scratch_shapes=scratch + sems,
        compiler_params=params(3),
        name="backward_part",
    )(*args)


def finish_kernel(*refs):
    srcs, part_h, dsts, small = refs[:6], refs[6], refs[7:13], refs[13:18]
    bufs, part, sem_in, sem_out = refs[18:24], refs[24], refs[25], refs[26]
    into = [pltpu.make_async_copy(a, b, sem_in.at[n]) for n, (a, b) in enumerate(zip(srcs, bufs))]
    into.append(pltpu.make_async_copy(part_h, part, sem_in.at[6]))
    out = [pltpu.make_async_copy(b, a, sem_out.at[n]) for n, (b, a) in enumerate(zip(bufs, dsts))]
    for c in into:
        c.start()
    for a, b in zip(into, out):
        a.wait()
        b.start()
    into[6].wait()
    small[0][...] = part[4 : 4 + PASSES_MAX, :]
    for n in range(4):
        small[1 + n][...] = part[n, :]
    for c in out:
        c.wait()


def finish_call(out, gi, part, gt, gq, gd, gu):
    share = part.shape[1]
    big = (out, gi, gt, gq, gd, gu)
    got = pl.pallas_call(
        finish_kernel,
        out_shape=tuple(struct(*v.shape) for v in big) + (struct(PASSES_MAX, share),) + (struct(share),) * 4,
        in_specs=[IN_HBM] * 7,
        out_specs=(IN_HBM,) * 6 + (IN_VMEM,) * 5,
        scratch_shapes=[vm(*v.shape) for v in big] + [vm(*part.shape)] + pairs(1, 7, 6),
        compiler_params=pltpu.CompilerParams(vmem_limit_bytes=63 << 20),
        name="finish_part",
    )(*big, part)
    return got[:2] + got[6:] + got[2:6]


def per_device(
    block_input, passes, pass_map, pass_table, gain_one, bias_one, w_qkv, w_out, gain_two, bias_two, w_up, w_down, grad_output
):
    x, go = block_input[0], grad_output[0]
    rows, feats = x.shape
    slots = rows * lax.axis_size("tensor")
    ways = lax.axis_size("dp")
    halving = ways == 8
    wq = jnp.transpose(w_qkv, (1, 2, 0))
    a, qc, kc, vc, o, lse, h1, c, dz = forward_call(
        passes, x, pass_table, gain_one, bias_one, gain_two, bias_two, go, wq, w_out, slots
    )
    dh1, vec2, zp, gd, gu = middle_call(h1, go, gain_two, c, dz, w_up, w_down, halving)
    got = backward_call(passes, x, pass_table, gain_one, h1, dh1, vec2, qc, kc, vc, o, lse, a, zp, wq, w_out, gd, gu, halving)
    out, gi, part, gt, gq = got[:5]
    if halving:
        out, gi, table, ga, ba, gb, bb, gt, gq, gd, gu = finish_call(out, gi, part, gt, gq, *got[5:])
    else:
        gd, gu = gd.reshape(feats, -1), gu.reshape(feats, -1)
        gt, gq, gu, gd = (lax.psum_scatter(v, "dp", scatter_dimension=0, tiled=True) for v in (gt, jnp.swapaxes(gq, 0, 1), gu, gd))
        part = lax.psum_scatter(part, "dp", scatter_dimension=1, tiled=True)
        gt, gq = gt.T, jnp.swapaxes(gq, 0, 1)
        table, ga, ba, gb, bb = part[4 : 4 + PASSES_MAX], part[0], part[1], part[2], part[3]
    return (
        out[None], gi[None], table, ga, ba, jnp.swapaxes(gq, 0, 1), gt, gb, bb, gu, gd.T,
    )


def solution(mesh):
    placed = (
        P("dp", "tensor", None), P("dp"), P("dp", "tensor"), P(), P(), P(), P(None, None, "tensor"), P("tensor", None),
        P(), P(), P(None, "tensor"), P("tensor", None), P("dp", "tensor", None),
    )
    return jax.shard_map(
        per_device,
        mesh=mesh,
        in_specs=placed,
        out_specs=(
            P("dp", "tensor", None), P("dp", "tensor", None), P(None, "dp"), P("dp"), P("dp"), P("dp", None, "tensor"),
            P("tensor", "dp"), P("dp"), P("dp"), P("dp", "tensor"), P("tensor", "dp"),
        ),
        check_vma=False,
    )
```
